1024 devices in a mesh: curve: 16 (over y, core), group: 64 (over z, x).
Axes of the slice: x: 8, y: 8, z: 8, core: 2. Of those that a mesh axis runs over, the one named last changes fastest.
Arguments:
- right_side: float32 [125, 524288], P(None, ('curve', 'group')), may hold values from -6 to 6, as said below
- conductivity: float32 [524288], P(('curve', 'group')), may hold values from 0.3 to 3
- destination: int32 [524288], P(('curve', 'group')), may hold values from 0 to 524287, as said below
- neighbour: int32 [6, 524288], P(None, ('curve', 'group')), may hold values from -1 to 1023, as said below
- orientation: int32 [6, 524288], P(None, ('curve', 'group')), may hold values from 0 to 3, as said below
- send_list: int32 [2, 262144], P(None, ('curve', 'group')), may hold values from 0 to 511, as said below
Outputs:
- solution: float32 [125, 524288], P(None, ('curve', 'group'))
- residual: float32 [125, 524288], P(None, ('curve', 'group'))
The draws below stay inside these ranges and needn't reach their ends.
Inputs may be any that keep to these rules, and one draw needn't show every extreme that they name: `right_side`: custom normal-like values. `destination`: A permutation of all cells. Devices are ordered along the curve with curve slowest; every cell's new device is its old device or the one just before or after it. From each device at most 64 cells go to the next device and exactly as many come back from it; 64 is reached at some pair of neighbouring devices in every draw. `neighbour`: values below 512 are local cells of the same device. Only face 0 may name a slot from 512 to 512 + 256 - 1 (filled by the previous device from its send_list row 1), only face 1 a slot from 768 up (filled by the next device from its send_list row 0). Faces are paired: the cell across face f sees this cell across face f xor 1. -1 only at the domain boundary; the first device has no partner across its face 0 slots and the last none across face 1 slots. `orientation`: both sides of a shared face carry the same code; ignored where neighbour is -1. `send_list`: per device 256 distinct local cells in each row.
All inputs are finite; a program needn't handle non-finite values.
Results may differ from the reference program's by a relative error of at most 0.00015.
Values sent between devices are 32-bit elements; how exact they have to be, the bound alone decides.
A program may use at most 32 MiB of HBM per device.

```python
import math
import jax
import jax.numpy as jnp
from jax import lax

CELLS_DEV = 512
SIDE = 16
NODES = 5
ITERS = 2
BLOCK = 125
GHOST = 256
MOVE = 64
RANKS = 1024
CELLS = 524288


def draw_right_side(key, part):
    key_rough = jax.random.fold_in(jax.random.fold_in(key, 3), 0)
    rough = jax.random.normal(key_rough, (BLOCK, CELLS), jnp.float32)
    return jnp.clip(rough, -6.0, 6.0)


def draw_destination(key, part):
    base_key = jax.random.fold_in(key, 29)
    key_swap, key_pick, key_rank, key_order = jax.random.split(base_key, 4)
    swap_counts = jax.random.randint(key_swap, (RANKS - 1,), 0, MOVE + 1).astype(jnp.int32)
    forced_at = jax.random.randint(key_pick, (), 0, RANKS - 1)
    swap_counts = swap_counts.at[forced_at].set(MOVE)
    zero_pad = jnp.zeros((1,), jnp.int32)
    to_left = jnp.concatenate([zero_pad, swap_counts])[:, None]
    to_right = jnp.concatenate([swap_counts, zero_pad])[:, None]
    local_rank = jax.vmap(lambda one_key: jax.random.permutation(one_key, CELLS_DEV))(jax.random.split(key_rank, RANKS)).astype(jnp.int32)
    old_owner = jnp.arange(RANKS, dtype=jnp.int32)[:, None]
    target = jnp.where(local_rank < to_left, old_owner - 1, jnp.where(local_rank >= CELLS_DEV - to_right, old_owner + 1, old_owner)).reshape(CELLS)
    shuffled = jax.random.permutation(key_order, CELLS).astype(jnp.int32)
    new_order = shuffled[jnp.argsort(target[shuffled], stable=True)]
    return jnp.zeros((CELLS,), jnp.int32).at[new_order].set(jnp.arange(CELLS, dtype=jnp.int32))


def mesh_arrays(key):
    base_key = jax.random.fold_in(key, 17)
    key_perm, key_code = jax.random.split(base_key)
    ghost_count = SIDE * SIDE
    layers = CELLS_DEV // ghost_count
    site_cell = jax.vmap(lambda one_key: jax.random.permutation(one_key, CELLS_DEV))(jax.random.split(key_perm, RANKS)).astype(jnp.int32)
    face_codes = jax.random.randint(key_code, (RANKS, CELLS_DEV, 3), 0, 4).astype(jnp.int32)
    site_ids = jnp.arange(CELLS_DEV, dtype=jnp.int32)
    layer_pos = (site_ids // ghost_count)[None, :]
    row_pos = (site_ids // SIDE % SIDE)[None, :]
    col_pos = (site_ids % SIDE)[None, :]
    plane_slot = row_pos * SIDE + col_pos
    rank_ids = jnp.arange(RANKS, dtype=jnp.int32)[:, None]

    def ahead_by(table, step):
        return jnp.roll(table, -step, axis=1)

    def behind_by(table, step):
        return jnp.roll(table, step, axis=1)
    face_zero = jnp.where(layer_pos > 0, behind_by(site_cell, ghost_count), jnp.where(rank_ids > 0, CELLS_DEV + plane_slot, -1))
    face_one = jnp.where(layer_pos < layers - 1, ahead_by(site_cell, ghost_count), jnp.where(rank_ids < RANKS - 1, CELLS_DEV + ghost_count + plane_slot, -1))
    face_two = jnp.where(row_pos > 0, behind_by(site_cell, SIDE), -1)
    face_three = jnp.where(row_pos < SIDE - 1, ahead_by(site_cell, SIDE), -1)
    face_four = jnp.where(col_pos > 0, behind_by(site_cell, 1), -1)
    face_five = jnp.where(col_pos < SIDE - 1, ahead_by(site_cell, 1), -1)
    code_x = face_codes[..., 0]
    code_y = face_codes[..., 1]
    code_z = face_codes[..., 2]
    previous_x = jnp.roll(jnp.roll(code_x, 1, axis=0), -(layers - 1) * ghost_count, axis=1)
    code_zero = jnp.where(layer_pos > 0, behind_by(code_x, ghost_count), previous_x)
    code_two = jnp.where(row_pos > 0, behind_by(code_y, SIDE), code_y)
    code_four = jnp.where(col_pos > 0, behind_by(code_z, 1), code_z)
    inverse = jnp.argsort(site_cell, axis=1, stable=True)
    neighbour_sites = jnp.stack([face_zero, face_one, face_two, face_three, face_four, face_five]).astype(jnp.int32)
    code_sites = jnp.stack([code_zero, code_x, code_two, code_y, code_four, code_z]).astype(jnp.int32)
    neighbour = jnp.take_along_axis(neighbour_sites, inverse[None], axis=2).reshape(6, CELLS)
    orientation = jnp.take_along_axis(code_sites, inverse[None], axis=2).reshape(6, CELLS)
    send_list = jnp.stack([site_cell[:, :ghost_count], site_cell[:, (layers - 1) * ghost_count:]]).reshape(2, RANKS * ghost_count)
    return (neighbour, orientation, send_list)


def draw_neighbour(key, part):
    return mesh_arrays(key)[0]


def draw_orientation(key, part):
    return mesh_arrays(key)[1]


def draw_send_list(key, part):
    return mesh_arrays(key)[2]


def levels(stream_key, dims, cuts, smallest, high):
    def one(dim, shards_of):
        heights = jax.random.uniform(jax.random.fold_in(jax.random.fold_in(stream_key, 6), dim), (shards_of,), jnp.float32, smallest / len(cuts), high / len(cuts))
        return jnp.repeat(jnp.exp(heights), dims[dim] // shards_of).reshape((-1,) + (1,) * (len(dims) - dim - 1))

    gain = one(*cuts[0])
    for cut in cuts[1:]:
        gain = gain * one(*cut)
    return gain


def setup_inputs(seed: int = 0) -> dict:
    arg_keys = jax.random.split(jax.random.key(seed), 7)
    right_side = draw_right_side(jax.random.fold_in(arg_keys[6], 71), 0)
    conductivity = jnp.clip(jnp.exp(math.log(3.0) - 2.3025851 * jax.random.uniform(arg_keys[1], (CELLS,), jnp.float32) ** levels(arg_keys[1], (CELLS,), ((0, 1024),), -0.2, 0.2)), 0.3, 3.0)
    destination = draw_destination(jax.random.fold_in(arg_keys[6], 71), 0)
    neighbour = draw_neighbour(jax.random.fold_in(arg_keys[6], 71), 0)
    orientation = draw_orientation(jax.random.fold_in(arg_keys[6], 71), 0)
    send_list = draw_send_list(jax.random.fold_in(arg_keys[6], 71), 0)
    return {"right_side": right_side, "conductivity": conductivity, "destination": destination, "neighbour": neighbour, "orientation": orientation, "send_list": send_list}


PENALTY = 80.0
HIGHEST = lax.Precision.HIGHEST
GAUSS_POINTS = (-0.9061798459386640, -0.5384693101056831, 0.0, 0.5384693101056831, 0.9061798459386640)
GAUSS_WEIGHTS = (0.2369268850561891, 0.4786286704993665, 0.5688888888888889, 0.4786286704993665, 0.2369268850561891)


def lagrange_value(points, position, location):
    product_value = 1.0
    for other_id in range(len(points)):
        if other_id != position:
            product_value = product_value * (location - points[other_id]) / (points[position] - points[other_id])
    return product_value


def lagrange_slope(points, position, location):
    slope_sum = 0.0
    for skipped in range(len(points)):
        if skipped == position:
            continue
        addend = 1.0 / (points[position] - points[skipped])
        for other_id in range(len(points)):
            if other_id != position and other_id != skipped:
                addend = addend * (location - points[other_id]) / (points[position] - points[other_id])
        slope_sum = slope_sum + addend
    return slope_sum


def basis_tables():
    points = [0.5 * (value + 1.0) for value in GAUSS_POINTS]
    weights = [0.5 * value for value in GAUSS_WEIGHTS]
    count = len(points)
    slopes = [[lagrange_slope(points, column, points[row_id]) for column in range(count)] for row_id in range(count)]
    start_value = [lagrange_value(points, column, 0.0) for column in range(count)]
    end_value = [lagrange_value(points, column, 1.0) for column in range(count)]
    start_slope = [-lagrange_slope(points, column, 0.0) for column in range(count)]
    end_slope = [lagrange_slope(points, column, 1.0) for column in range(count)]
    listed = (weights, slopes, start_value, end_value, start_slope, end_slope)
    return tuple(jnp.asarray(table, jnp.float32) for table in listed)


def face_vectors(face_id, tables):
    if face_id % 2:
        return tables[3], tables[5]
    return tables[2], tables[4]


def face_data(block_field, conduct, face_id, tables):
    trace_vec, normal_vec = face_vectors(face_id, tables)
    axis_id = face_id // 2
    trace_value = jnp.tensordot(trace_vec, block_field, axes=([0], [axis_id]), precision=HIGHEST)
    trace_flux = conduct * jnp.tensordot(normal_vec, block_field, axes=([0], [axis_id]), precision=HIGHEST)
    return trace_value, trace_flux


def spread_back(vector, face_part, axis_id):
    bcast_shape = [1, 1, 1, 1]
    bcast_shape[axis_id] = NODES
    return vector.reshape(bcast_shape) * jnp.expand_dims(face_part, axis_id)


def volume_term(block_field, conduct, tables):
    weights, slopes = tables[0], tables[1]
    weight_3d = (weights[:, None, None] * weights[None, :, None] * weights[None, None, :])[..., None]
    result = weight_3d * block_field
    forward = ("qp,pjkc->qjkc", "qp,ipkc->iqkc", "qp,ijpc->ijqc")
    backward = ("qp,qjkc->pjkc", "qp,iqkc->ipkc", "qp,ijqc->ijpc")
    for axis_id in range(3):
        grads = jnp.einsum(forward[axis_id], slopes, block_field, precision=HIGHEST)
        result = result + jnp.einsum(backward[axis_id], slopes, weight_3d * conduct * grads, precision=HIGHEST)
    return result


def face_term(trace_value, trace_flux, conduct, other_value, other_flux, other_conduct, partner, orient_code, face_id, tables):
    weights = tables[0]
    trace_vec, normal_vec = face_vectors(face_id, tables)
    axis_id = face_id // 2
    flip_first = (orient_code % 2) == 1
    flip_second = (orient_code // 2) == 1
    other_value = jnp.where(flip_first, other_value[::-1], other_value)
    other_value = jnp.where(flip_second, other_value[:, ::-1], other_value)
    other_flux = jnp.where(flip_first, other_flux[::-1], other_flux)
    other_flux = jnp.where(flip_second, other_flux[:, ::-1], other_flux)
    outside = partner < 0
    other_value = jnp.where(outside, -trace_value, other_value)
    other_flux = jnp.where(outside, -trace_flux, other_flux)
    other_conduct = jnp.where(outside, conduct, other_conduct)
    penalty = PENALTY * jnp.maximum(conduct, other_conduct)
    trace_jump = trace_value - other_value
    mean_flux = 0.5 * (trace_flux - other_flux)
    face_weight = (weights[:, None] * weights[None, :])[:, :, None]
    first_part = spread_back(trace_vec, face_weight * (penalty * trace_jump - mean_flux), axis_id)
    return first_part + spread_back(normal_vec, face_weight * (-0.5 * conduct * trace_jump), axis_id)


def global_partners(neighbour, send_list):
    cell_ids = jnp.arange(CELLS, dtype=jnp.int32)
    owner = cell_ids // CELLS_DEV
    lower = jnp.maximum(owner - 1, 0)
    upper = jnp.minimum(owner + 1, RANKS - 1)
    left_slot = jnp.clip(neighbour - CELLS_DEV, 0, GHOST - 1)
    right_slot = jnp.clip(neighbour - CELLS_DEV - GHOST, 0, GHOST - 1)
    from_left = lower * CELLS_DEV + send_list[1][lower * GHOST + left_slot]
    from_right = upper * CELLS_DEV + send_list[0][upper * GHOST + right_slot]
    local_ids = owner * CELLS_DEV + neighbour
    joined = jnp.where(neighbour < CELLS_DEV, local_ids, jnp.where(neighbour < CELLS_DEV + GHOST, from_left, from_right))
    return jnp.where(neighbour < 0, -1, joined).astype(jnp.int32)


def operate(block_field, conduct, partners, orientation, tables):
    faces = [face_data(block_field, conduct, face_id, tables) for face_id in range(6)]
    result = volume_term(block_field, conduct, tables)
    for face_id in range(6):
        partner = partners[face_id]
        safe_idx = jnp.where(partner < 0, 0, partner)
        other_value, other_flux = faces[face_id ^ 1]
        result = result + face_term(faces[face_id][0], faces[face_id][1], conduct,
                                    other_value[:, :, safe_idx], other_flux[:, :, safe_idx], conduct[safe_idx],
                                    partner, orientation[face_id], face_id, tables)
    return result


def reference(right_side, conductivity, destination, neighbour, orientation, send_list):
    tables = basis_tables()
    placed = jnp.zeros((BLOCK, CELLS), jnp.float32).at[:, destination].set(right_side)
    conduct = jnp.zeros((CELLS,), jnp.float32).at[destination].set(conductivity)
    partners = global_partners(neighbour, send_list)
    source = placed.reshape(NODES, NODES, NODES, CELLS)
    solution = jnp.zeros_like(source)
    residual = source
    direction = source
    norm_now = jnp.sum(residual * residual)
    for step in range(ITERS):
        image = operate(direction, conduct, partners, orientation, tables)
        step_size = norm_now / jnp.sum(direction * image)
        solution = solution + step_size * direction
        residual = residual - step_size * image
        if step + 1 < ITERS:
            norm_next = jnp.sum(residual * residual)
            direction = residual + (norm_next / norm_now) * direction
            norm_now = norm_next
    return solution.reshape(BLOCK, CELLS), residual.reshape(BLOCK, CELLS)
```

```python
import functools

import jax
import jax.numpy as jnp
import ml_dtypes
import numpy as np
from jax import lax
from jax.experimental import pallas as pl
from jax.experimental.pallas import tpu as pltpu
from jax.sharding import PartitionSpec as P

NODES = 5
BLOCK = 125
CELLS = 512
GHOST = 256
MOVE = 64
PENALTY = 80.0
FACE = 64
HALF = 32
ROWS = 128
X_SIZE = 8
MESH = pl.DeviceIdType.MESH
F32 = jnp.float32
BF16 = jnp.bfloat16
CURVE_GROUP = ("curve", "group")
GAUSS_POINTS = (-0.906179845938664, -0.5384693101056831, 0.0, 0.5384693101056831, 0.906179845938664)
GAUSS_WEIGHTS = (
    0.2369268850561891,
    0.4786286704993665,
    0.5688888888888889,
    0.4786286704993665,
    0.2369268850561891,
)


def lagrange_value(points, position, location):
    product_value = 1.0
    for other in range(len(points)):
        if other != position:
            product_value *= (location - points[other]) / (points[position] - points[other])
    return product_value


def lagrange_slope(points, position, location):
    slope_sum = 0.0
    for skipped in range(len(points)):
        if skipped == position:
            continue
        addend = 1.0 / (points[position] - points[skipped])
        for other in range(len(points)):
            if other != position and other != skipped:
                addend *= (location - points[other]) / (points[position] - points[other])
        slope_sum += addend
    return slope_sum


def along_axis(matrix, axis_id):
    eye = np.eye(NODES)
    parts = [eye, eye, eye]
    parts[axis_id] = matrix
    return np.kron(parts[0], np.kron(parts[1], parts[2]))


def tables():
    points = [0.5 * (value + 1.0) for value in GAUSS_POINTS]
    weights = np.array([0.5 * value for value in GAUSS_WEIGHTS])
    slopes = np.array([[lagrange_slope(points, p, points[q]) for p in range(NODES)] for q in range(NODES)])
    ends = [
        (
            np.array([lagrange_value(points, p, 0.0) for p in range(NODES)]),
            np.array([-lagrange_slope(points, p, 0.0) for p in range(NODES)]),
        ),
        (
            np.array([lagrange_value(points, p, 1.0) for p in range(NODES)]),
            np.array([lagrange_slope(points, p, 1.0) for p in range(NODES)]),
        ),
    ]
    cell_weight = np.kron(weights, np.kron(weights, weights))
    volume = sum(
        along_axis(slopes, a).T @ (cell_weight[:, None] * along_axis(slopes, a)) for a in range(3)
    )
    root = np.sqrt(0.5)
    modes = np.array(
        [
            [root, 0, 0, 0, root],
            [0, root, 0, root, 0],
            [0, 0, 1, 0, 0],
            [root, 0, 0, 0, -root],
            [0, root, 0, -root, 0],
        ]
    )
    modes = np.kron(modes, modes)
    mode_weight = np.array([weights[0], weights[1], weights[2], weights[0], weights[1]])
    mode_weight = np.kron(mode_weight, mode_weight)
    forward = np.zeros((6 * FACE + ROWS, ROWS))
    backward = np.zeros((ROWS, 6 * FACE))
    for face in range(6):
        trace, normal = ends[face % 2]
        trace = modes @ along_axis(trace[None, :], face // 2)
        normal = modes @ along_axis(normal[None, :], face // 2)
        row = face * FACE
        forward[row : row + 25, :BLOCK] = trace
        forward[row + 25, BLOCK] = 1.0
        forward[row + HALF : row + HALF + 25, :BLOCK] = normal
        backward[:BLOCK, row : row + 25] = trace.T * mode_weight
        backward[:BLOCK, row + HALF : row + HALF + 25] = -0.5 * normal.T * mode_weight
    forward[6 * FACE : 6 * FACE + BLOCK, :BLOCK] = volume
    weight_rows = np.zeros((ROWS, 1))
    weight_rows[:BLOCK, 0] = cell_weight

    def halves(table):
        high = table.astype(ml_dtypes.bfloat16)
        return high, (table - high.astype(np.float64)).astype(ml_dtypes.bfloat16)

    fwd_high, fwd_low = halves(forward)
    back_high, back_low = halves(backward)
    return (
        np.concatenate([fwd_high, fwd_high], 1),
        fwd_low,
        back_high,
        back_low,
        np.broadcast_to(weight_rows, (ROWS, 128)).astype(np.float32),
    )


def dot_nn(left, right):
    return jnp.dot(left, right, preferred_element_type=F32)


def dot_nt(left, right):
    return lax.dot_general(left, right, (((1,), (1,)), ((), ())), preferred_element_type=F32)


def split2(value):
    high = value.astype(BF16)
    return high, (value - high.astype(F32)).astype(BF16)


def split3(value):
    high = value.astype(BF16)
    rest = value - high.astype(F32)
    mid = rest.astype(BF16)
    return high, mid, (rest - mid.astype(F32)).astype(BF16)


def onehot(index_row, rows, start=0):
    ids = lax.broadcasted_iota(jnp.int32, (rows, index_row.shape[1]), 0) + start
    return jnp.where(ids == index_row, 1.0, 0.0).astype(BF16)


def kernel(
    n_curve, n_group, x_size,
    rs_ref, cond_ref, dest_ref, nb_ref, ori_ref, sl_ref, fa_ref, fb_ref, bh_ref, bl_ref, w_ref,
    b_out, y_out, z_out, coef_out,
    x_ref, x3_ref, q_ref, g_ref, gg_ref, s_ref, sign_ref, f_ref, fs_ref, ch_ref, cl_ref,
    mig_send, mig_recv, halo_send, halo_recv, row_send, curve_recv, x_recv, z_recv,
    mig_ssem, mig_rsem, halo_ssem, halo_rsem, curve_ssem, curve_rsem, x_ssem, x_rsem, z_ssem, z_rsem,
):
    curve = lax.axis_index("curve")
    group = lax.axis_index("group")
    me = curve * n_group + group
    total = n_curve * n_group
    left_rank = lax.rem(me + total - 1, total)
    right_rank = lax.rem(me + 1, total)

    def device(rank):
        return (rank // n_group, lax.rem(rank, n_group))

    left, right = device(left_rank), device(right_rank)
    z_size = n_group // x_size
    x_pos = lax.rem(group, x_size)
    z_pos = group // x_size
    curve_peers = [(lax.rem(curve + d, n_curve), group) for d in range(1, n_curve)]
    x_peers = [(curve, z_pos * x_size + lax.rem(x_pos + d, x_size)) for d in range(1, x_size)]
    z_peers = [(curve, lax.rem(z_pos + d, z_size) * x_size + x_pos) for d in range(1, z_size)]
    everyone = [left, right] + curve_peers + x_peers + z_peers

    barrier = pltpu.get_barrier_semaphore()
    for peer in everyone:
        pl.semaphore_signal(barrier, inc=1, device_id=peer, device_id_type=MESH)

    destination = dest_ref[...]
    target = lax.shift_right_arithmetic(destination, 9) - me
    slot = jnp.bitwise_and(destination, CELLS - 1)
    x_ref[0:BLOCK, :] = rs_ref[...]
    x_ref[BLOCK : BLOCK + 1, :] = cond_ref[...]
    x_ref[BLOCK + 1 : BLOCK + 2, :] = (slot + 1).astype(F32)
    x_ref[BLOCK + 2 : ROWS, :] = jnp.zeros((ROWS - BLOCK - 2, CELLS), F32)
    high, mid, low = split3(x_ref[...])
    x3_ref[0:ROWS, :] = high
    x3_ref[ROWS : 2 * ROWS, :] = mid
    x3_ref[2 * ROWS : 3 * ROWS, :] = low
    row8 = lax.broadcasted_iota(jnp.int32, (8, CELLS), 0)
    leaving = jnp.where(((row8 == 0) & (target == -1)) | ((row8 == 1) & (target == 1)), 1.0, 0.0)
    for start in range(0, CELLS, 64):
        ids = lax.broadcasted_iota(jnp.int32, (64, CELLS), 0) + start
        lanes = lax.broadcasted_iota(jnp.int32, (64, CELLS), 1)
        q_ref[start : start + 64, :] = jnp.where(ids <= lanes, 1.0, 0.0).astype(BF16)
    counts = dot_nn(leaving.astype(BF16), q_ref[...]).astype(jnp.int32)
    place = jnp.where(target == -1, counts[0:1] - 1, jnp.where(target == 1, counts[1:2] + (MOVE - 1), -1))
    packed = dot_nt(onehot(place, 2 * MOVE), x3_ref[...])
    mig_send[...] = packed[:, 0:ROWS] + packed[:, ROWS : 2 * ROWS] + packed[:, 2 * ROWS :]

    pl.semaphore_wait(barrier, len(everyone))

    def copy(source, sink, ssem, rsem, peer):
        return pltpu.make_async_remote_copy(
            src_ref=source, dst_ref=sink, send_sem=ssem, recv_sem=rsem, device_id=peer, device_id_type=MESH
        )

    to_left = copy(
        mig_send.at[pl.ds(0, MOVE)], mig_recv.at[pl.ds(MOVE, MOVE)], mig_ssem.at[0], mig_rsem.at[0], left
    )
    to_right = copy(
        mig_send.at[pl.ds(MOVE, MOVE)], mig_recv.at[pl.ds(0, MOVE)], mig_ssem.at[1], mig_rsem.at[1], right
    )
    to_left.start()
    to_right.start()

    staying = jnp.where(target == 0, slot, -1)
    for start in range(0, CELLS, 64):
        q_ref[start : start + 64, :] = onehot(staying, 64, start)
    stay = dot_nt(x3_ref[...], q_ref[...])
    f_ref[0:ROWS, :] = stay[0:ROWS] + stay[ROWS : 2 * ROWS] + stay[2 * ROWS :]

    for side in range(2):
        for start in range(0, CELLS, 128):
            s_ref[side, start : start + 128, :] = onehot(sl_ref[side : side + 1, :], 128, start)
    mode = lax.broadcasted_iota(jnp.int32, (HALF, CELLS), 0)
    odd_first = jnp.where((mode >= 15) & (mode < 25), 2.0, 0.0)
    second = functools.reduce(jnp.logical_or, [mode == 5 * i + j for i in range(5) for j in (3, 4)])
    odd_second = jnp.where(second, 2.0, 0.0)
    outside = []
    for face in range(6):
        partner = nb_ref[face : face + 1, :]
        outside.append(jnp.where(partner < 0, 2.0, 1.0))
        for start in range(0, CELLS, 64):
            g_ref[face, start : start + 64, :] = onehot(partner, 64, start)
        if face < 2:
            for start in range(0, GHOST, 64):
                gg_ref[face, start : start + 64, :] = onehot(partner, 64, CELLS + face * GHOST + start)
        code = ori_ref[face : face + 1, :]
        first_bit = jnp.bitwise_and(code, 1).astype(F32)
        second_bit = lax.shift_right_arithmetic(code, 1).astype(F32)
        sign_ref[face] = (1.0 - odd_first * first_bit) * (1.0 - odd_second * second_bit)

    to_left.wait_recv()
    to_right.wait_recv()
    arrived = mig_recv[...].T
    place_in = arrived[BLOCK + 1 : BLOCK + 2, :].astype(jnp.int32) - 1
    for start in range(0, CELLS, 128):
        q_ref[start : start + 128, 0 : 2 * MOVE] = onehot(place_in, 128, start)
    parts = jnp.concatenate(split3(arrived), 0)
    moved = dot_nt(parts, q_ref[:, 0 : 2 * MOVE])
    field = f_ref[0:ROWS, :] + (moved[0:ROWS] + moved[ROWS : 2 * ROWS] + moved[2 * ROWS :])
    conduct = field[BLOCK : BLOCK + 1, :]
    row_ids = lax.broadcasted_iota(jnp.int32, (ROWS, CELLS), 0)
    source = jnp.where(row_ids < BLOCK, field, 0.0)
    b_out[...] = source

    def operate(value, step):
        high, low = split2(jnp.where(row_ids == BLOCK, conduct, value))
        both = jnp.concatenate([high, low], 0)

        def forward(start, stop):
            rows = pl.ds(start, stop - start)
            f_ref[rows, :] = dot_nn(fa_ref[rows, :], both) + dot_nn(fb_ref[rows, :], high)

        def stack(face):
            high, low = split2(f_ref[face * FACE : (face + 1) * FACE, :])
            fs_ref[face, 0:FACE, :] = high
            fs_ref[face, FACE : 2 * FACE, :] = low

        def pair(product):
            return product[0:FACE] + product[FACE : 2 * FACE]

        copies = []
        forward(0, 2 * FACE)
        for side, peer in ((0, left), (1, right)):
            stack(side)
            halo_send[step, side] = pair(dot_nn(fs_ref[side], s_ref[side]))
            copies.append(
                copy(
                    halo_send.at[step, side], halo_recv.at[step, 1 - side],
                    halo_ssem.at[step, side], halo_rsem.at[step, side], peer,
                )
            )
            copies[-1].start()
        forward(2 * FACE, 6 * FACE + ROWS)
        for face in range(2, 6):
            stack(face)

        def coefficients(face, near):
            row = face * FACE
            trace = f_ref[row : row + HALF, :]
            normal = f_ref[row + HALF : row + FACE, :]
            near_conduct = near[25:26, :]
            sign = sign_ref[face]
            near_value = sign * near[0:HALF]
            near_normal = sign * near[HALF:FACE]
            penalty = PENALTY * jnp.maximum(conduct, near_conduct)
            jump = outside[face] * trace - near_value
            first = (
                penalty * jump
                - (0.5 * outside[face] * conduct) * normal
                + (0.5 * near_conduct) * near_normal
            )
            for offset, part in ((0, first), (HALF, conduct * jump)):
                high, low = split2(part)
                ch_ref[row + offset : row + offset + HALF, :] = high
                cl_ref[row + offset : row + offset + HALF, :] = low

        def backward(start, stop):
            columns = slice(start * FACE, stop * FACE)
            back_high = bh_ref[:, columns]
            return (
                dot_nn(back_high, ch_ref[columns, :])
                + dot_nn(back_high, cl_ref[columns, :])
                + dot_nn(bl_ref[:, columns], ch_ref[columns, :])
            )

        for face in range(2, 6):
            coefficients(face, pair(dot_nn(fs_ref[face ^ 1], g_ref[face])))
        local = [pair(dot_nn(fs_ref[face ^ 1], g_ref[face])) for face in range(2)]
        result = w_ref[:, 0:1] * value + conduct * f_ref[6 * FACE :, :] + backward(2, 6)
        for face in range(2):
            copies[1 - face].wait_recv()
            high, low = split2(halo_recv[step, face])
            ghost = pair(dot_nn(jnp.concatenate([high, low], 0), gg_ref[face]))
            coefficients(face, local[face] + ghost)
        return result + backward(0, 2), copies

    image, copies_one = operate(source, 0)
    y_out[...] = image
    second_image, copies_two = operate(image, 1)
    z_out[...] = second_image

    source = b_out[...]
    image = y_out[...]
    lane = lax.broadcasted_iota(jnp.int32, (1, 128), 1)
    row = jnp.zeros((1, 128), F32)
    for index, terms in enumerate(
        (source * source, source * image, image * image, source * second_image, image * second_image)
    ):
        row = row + jnp.where(lane == index, jnp.sum(terms, axis=(0, 1), keepdims=True), 0.0)

    sent = []
    for phase, (peers, landing, ssem, rsem) in enumerate(
        (
            (curve_peers, curve_recv, curve_ssem, curve_rsem),
            (x_peers, x_recv, x_ssem, x_rsem),
            (z_peers, z_recv, z_ssem, z_rsem),
        )
    ):
        row_send[phase] = row
        out = [
            copy(row_send.at[phase], landing.at[i], ssem.at[i], rsem.at[i], peer)
            for i, peer in enumerate(peers)
        ]
        for one in out:
            one.start()
        for i, one in enumerate(out):
            one.wait_recv()
            row = row + landing[i]
        sent += out

    bb, by, yy, bz, yz = (
        jnp.sum(jnp.where(lane == index, row, 0.0), axis=1, keepdims=True) for index in range(5)
    )
    alpha = bb / by
    norm_next = bb - alpha * (2.0 * by - alpha * yy)
    beta = norm_next / bb
    grow = 1.0 + beta
    curvature = grow * (grow * by - alpha * (bz + yy)) + alpha * (alpha * yz)
    alpha_next = norm_next / curvature
    coef_out[0:1, :] = jnp.broadcast_to(alpha + alpha_next * grow, (1, 128))
    coef_out[1:2, :] = jnp.broadcast_to(alpha * alpha_next, (1, 128))
    for one in [to_left, to_right] + copies_one + copies_two + sent:
        one.wait_send()


def solution(mesh):
    n_curve, n_group = mesh.shape["curve"], mesh.shape["group"]
    x_size = min(X_SIZE, n_group)
    z_size = n_group // x_size
    constants = tables()
    field = jax.ShapeDtypeStruct((ROWS, CELLS), F32)
    call = pl.pallas_call(
        functools.partial(kernel, n_curve, n_group, x_size),
        out_shape=(field, field, field, jax.ShapeDtypeStruct((2, 128), F32)),
        in_specs=[pl.BlockSpec(memory_space=pltpu.VMEM)] * 11,
        out_specs=[pl.BlockSpec(memory_space=pltpu.VMEM)] * 4,
        scratch_shapes=[
            pltpu.VMEM((ROWS, CELLS), F32),
            pltpu.VMEM((3 * ROWS, CELLS), BF16),
            pltpu.VMEM((CELLS, CELLS), BF16),
            pltpu.VMEM((6, CELLS, CELLS), BF16),
            pltpu.VMEM((2, GHOST, CELLS), BF16),
            pltpu.VMEM((2, CELLS, GHOST), BF16),
            pltpu.VMEM((6, HALF, CELLS), F32),
            pltpu.VMEM((6 * FACE + ROWS, CELLS), F32),
            pltpu.VMEM((6, 2 * FACE, CELLS), BF16),
            pltpu.VMEM((6 * FACE, CELLS), BF16),
            pltpu.VMEM((6 * FACE, CELLS), BF16),
            pltpu.VMEM((2 * MOVE, ROWS), F32),
            pltpu.VMEM((2 * MOVE, ROWS), F32),
            pltpu.VMEM((2, 2, FACE, GHOST), F32),
            pltpu.VMEM((2, 2, FACE, GHOST), F32),
            pltpu.VMEM((3, 1, 128), F32),
            pltpu.VMEM((n_curve - 1, 1, 128), F32),
            pltpu.VMEM((x_size - 1, 1, 128), F32),
            pltpu.VMEM((z_size - 1, 1, 128), F32),
            pltpu.SemaphoreType.DMA((2,)),
            pltpu.SemaphoreType.DMA((2,)),
            pltpu.SemaphoreType.DMA((2, 2)),
            pltpu.SemaphoreType.DMA((2, 2)),
            pltpu.SemaphoreType.DMA((n_curve - 1,)),
            pltpu.SemaphoreType.DMA((n_curve - 1,)),
            pltpu.SemaphoreType.DMA((x_size - 1,)),
            pltpu.SemaphoreType.DMA((x_size - 1,)),
            pltpu.SemaphoreType.DMA((z_size - 1,)),
            pltpu.SemaphoreType.DMA((z_size - 1,)),
        ],
        compiler_params=pltpu.CompilerParams(collective_id=0, has_side_effects=True),
    )

    def body(right_side, conductivity, destination, neighbour, orientation, send_list):
        b, y, z, coef = call(
            right_side, conductivity[None], destination[None], neighbour, orientation, send_list,
            *[jnp.asarray(table) for table in constants],
        )
        b, y, z = b[:BLOCK], y[:BLOCK], z[:BLOCK]
        first, second = coef[0, 0], coef[1, 0]
        return first * b - second * y, b - first * y + second * z

    in_specs = (
        P(None, CURVE_GROUP),
        P(CURVE_GROUP),
        P(CURVE_GROUP),
        P(None, CURVE_GROUP),
        P(None, CURVE_GROUP),
        P(None, CURVE_GROUP),
    )
    out_specs = (P(None, CURVE_GROUP), P(None, CURVE_GROUP))
    return jax.shard_map(body, mesh=mesh, in_specs=in_specs, out_specs=out_specs, check_vma=False)
```

```python
import functools

import jax
import jax.numpy as jnp
import ml_dtypes
import numpy as np
from jax import lax
from jax.experimental import pallas as pl
from jax.experimental.pallas import tpu as pltpu
from jax.sharding import PartitionSpec as P

NODES = 5
BLOCK = 125
CELLS = 512
GHOST = 256
MOVE = 64
PENALTY = 80.0
FACE = 64
HALF = 32
ROWS = 128
X_SIZE = 8
MESH = pl.DeviceIdType.MESH
F32 = jnp.float32
BF16 = jnp.bfloat16
CURVE_GROUP = ("curve", "group")
GAUSS_POINTS = (-0.906179845938664, -0.5384693101056831, 0.0, 0.5384693101056831, 0.906179845938664)
GAUSS_WEIGHTS = (
    0.2369268850561891,
    0.4786286704993665,
    0.5688888888888889,
    0.4786286704993665,
    0.2369268850561891,
)


def lagrange_value(points, position, location):
    product_value = 1.0
    for other in range(len(points)):
        if other != position:
            product_value *= (location - points[other]) / (points[position] - points[other])
    return product_value


def lagrange_slope(points, position, location):
    slope_sum = 0.0
    for skipped in range(len(points)):
        if skipped == position:
            continue
        addend = 1.0 / (points[position] - points[skipped])
        for other in range(len(points)):
            if other != position and other != skipped:
                addend *= (location - points[other]) / (points[position] - points[other])
        slope_sum += addend
    return slope_sum


def along_axis(matrix, axis_id):
    eye = np.eye(NODES)
    parts = [eye, eye, eye]
    parts[axis_id] = matrix
    return np.kron(parts[0], np.kron(parts[1], parts[2]))


def tables():
    points = [0.5 * (value + 1.0) for value in GAUSS_POINTS]
    weights = np.array([0.5 * value for value in GAUSS_WEIGHTS])
    slopes = np.array([[lagrange_slope(points, p, points[q]) for p in range(NODES)] for q in range(NODES)])
    ends = [
        (
            np.array([lagrange_value(points, p, 0.0) for p in range(NODES)]),
            np.array([-lagrange_slope(points, p, 0.0) for p in range(NODES)]),
        ),
        (
            np.array([lagrange_value(points, p, 1.0) for p in range(NODES)]),
            np.array([lagrange_slope(points, p, 1.0) for p in range(NODES)]),
        ),
    ]
    cell_weight = np.kron(weights, np.kron(weights, weights))
    volume = sum(
        along_axis(slopes, a).T @ (cell_weight[:, None] * along_axis(slopes, a)) for a in range(3)
    )
    root = np.sqrt(0.5)
    modes = np.array(
        [
            [root, 0, 0, 0, root],
            [0, root, 0, root, 0],
            [0, 0, 1, 0, 0],
            [root, 0, 0, 0, -root],
            [0, root, 0, -root, 0],
        ]
    )
    modes = np.kron(modes, modes)
    mode_weight = np.array([weights[0], weights[1], weights[2], weights[0], weights[1]])
    mode_weight = np.kron(mode_weight, mode_weight)
    forward = np.zeros((6 * FACE + ROWS, ROWS))
    backward = np.zeros((ROWS, 6 * FACE))
    for face in range(6):
        trace, normal = ends[face % 2]
        trace = modes @ along_axis(trace[None, :], face // 2)
        normal = modes @ along_axis(normal[None, :], face // 2)
        row = face * FACE
        forward[row : row + 25, :BLOCK] = trace
        forward[row + 25, BLOCK] = 1.0
        forward[row + HALF : row + HALF + 25, :BLOCK] = normal
        backward[:BLOCK, row : row + 25] = trace.T * mode_weight
        backward[:BLOCK, row + HALF : row + HALF + 25] = -0.5 * normal.T * mode_weight
    forward[6 * FACE : 6 * FACE + BLOCK, :BLOCK] = volume
    weight_rows = np.zeros((ROWS, 1))
    weight_rows[:BLOCK, 0] = cell_weight

    def halves(table):
        high = table.astype(ml_dtypes.bfloat16)
        return high, (table - high.astype(np.float64)).astype(ml_dtypes.bfloat16)

    fwd_high, fwd_low = halves(forward)
    back_high, back_low = halves(backward)
    return (
        np.concatenate([fwd_high, fwd_high], 1),
        fwd_low,
        back_high,
        back_low,
        np.broadcast_to(weight_rows, (ROWS, 128)).astype(np.float32),
    )


def dot_nn(left, right):
    return jnp.dot(left, right, preferred_element_type=F32)


def dot_nt(left, right):
    return lax.dot_general(left, right, (((1,), (1,)), ((), ())), preferred_element_type=F32)


def split2(value):
    high = value.astype(BF16)
    return high, (value - high.astype(F32)).astype(BF16)


def split3(value):
    high = value.astype(BF16)
    rest = value - high.astype(F32)
    mid = rest.astype(BF16)
    return high, mid, (rest - mid.astype(F32)).astype(BF16)


def onehot(index_row, rows, start=0):
    ids = lax.broadcasted_iota(jnp.int32, (rows, index_row.shape[1]), 0) + start
    return jnp.where(ids == index_row, 1.0, 0.0).astype(BF16)


def kernel(
    n_curve, n_group, x_size,
    rs_hbm, cond_hbm, dest_hbm, nb_hbm, ori_hbm, sl_hbm, fa_hbm, fb_hbm, bh_hbm, bl_hbm, w_hbm,
    solution_out, residual_out,
    rs_ref, cond_ref, dest_ref, nb_ref, ori_ref, sl_ref, fa_ref, fb_ref, bh_ref, bl_ref, w_ref, load_sem,
    b_ref, y_ref, tail_ref, x3_ref, q_ref, g_ref, gg_ref, s_ref, sign_ref, f_ref, fs_ref, ch_ref, cl_ref,
    mig_send, mig_recv, halo_send, halo_recv, row_send, curve_recv, x_recv, z_recv,
    mig_ssem, mig_rsem, halo_ssem, halo_rsem, curve_ssem, curve_rsem, x_ssem, x_rsem, z_ssem, z_rsem,
):
    curve = lax.axis_index("curve")
    group = lax.axis_index("group")
    me = curve * n_group + group
    total = n_curve * n_group
    has_left, has_right = me > 0, me < total - 1

    def device(rank):
        return (rank // n_group, lax.rem(rank, n_group))

    left, right = device(lax.rem(me + total - 1, total)), device(lax.rem(me + 1, total))
    z_size = n_group // x_size
    x_pos = lax.rem(group, x_size)
    z_pos = group // x_size
    curve_peers = [(lax.rem(curve + d, n_curve), group) for d in range(1, n_curve)]
    x_peers = [(curve, z_pos * x_size + lax.rem(x_pos + d, x_size)) for d in range(1, x_size)]
    z_peers = [(curve, lax.rem(z_pos + d, z_size) * x_size + x_pos) for d in range(1, z_size)]
    everyone = curve_peers + x_peers + z_peers

    barrier = pltpu.get_barrier_semaphore()
    for peer in everyone:
        pl.semaphore_signal(barrier, inc=1, device_id=peer, device_id_type=MESH)

    @pl.when(has_left)
    def _():
        pl.semaphore_signal(barrier, inc=1, device_id=left, device_id_type=MESH)

    @pl.when(has_right)
    def _():
        pl.semaphore_signal(barrier, inc=1, device_id=right, device_id_type=MESH)

    loads = {}
    for i, (name, source, sink) in enumerate(
        (
            ("dest", dest_hbm, dest_ref),
            ("rs", rs_hbm, rs_ref),
            ("cond", cond_hbm, cond_ref),
            ("nb", nb_hbm, nb_ref),
            ("sl", sl_hbm, sl_ref),
            ("ori", ori_hbm, ori_ref),
            ("fa", fa_hbm, fa_ref),
            ("fb", fb_hbm, fb_ref),
            ("bh", bh_hbm, bh_ref),
            ("bl", bl_hbm, bl_ref),
            ("w", w_hbm, w_ref),
        )
    ):
        loads[name] = pltpu.make_async_copy(source, sink, load_sem.at[i])
        loads[name].start()
    for start in range(0, CELLS, 64):
        ids = lax.broadcasted_iota(jnp.int32, (64, CELLS), 0) + start
        lanes = lax.broadcasted_iota(jnp.int32, (64, CELLS), 1)
        q_ref[start : start + 64, :] = jnp.where(ids <= lanes, 1.0, 0.0).astype(BF16)

    @pl.when(jnp.logical_not(has_left))
    def _():
        mig_recv[0:MOVE, :] = jnp.zeros((MOVE, ROWS), F32)
        halo_recv[:, 0] = jnp.zeros((2, FACE, GHOST), F32)

    @pl.when(jnp.logical_not(has_right))
    def _():
        mig_recv[MOVE:, :] = jnp.zeros((MOVE, ROWS), F32)
        halo_recv[:, 1] = jnp.zeros((2, FACE, GHOST), F32)

    loads["dest"].wait()

    destination = dest_ref[...]
    target = lax.shift_right_arithmetic(destination, 9) - me
    slot = jnp.bitwise_and(destination, CELLS - 1)
    row8 = lax.broadcasted_iota(jnp.int32, (8, CELLS), 0)
    leaving = jnp.where(((row8 == 0) & (target == -1)) | ((row8 == 1) & (target == 1)), 1.0, 0.0)
    counts = dot_nn(leaving.astype(BF16), q_ref[...]).astype(jnp.int32)
    place = jnp.where(target == -1, counts[0:1] - 1, jnp.where(target == 1, counts[1:2] + (MOVE - 1), -1))
    loads["rs"].wait()
    loads["cond"].wait()
    tail_ref[0:13, :] = rs_ref[112:BLOCK, :]
    tail_ref[13:14, :] = cond_ref[...]
    tail_ref[14:15, :] = (slot + 1).astype(F32)
    tail_ref[15:16, :] = jnp.zeros((1, CELLS), F32)
    for start, stop, value in ((0, 112, rs_ref[0:112, :]), (112, ROWS, tail_ref[...])):
        for i, part in enumerate(split3(value)):
            x3_ref[i * ROWS + start : i * ROWS + stop, :] = part
    packed = dot_nt(onehot(place, 2 * MOVE), x3_ref[...])
    mig_send[...] = packed[:, 0:ROWS] + packed[:, ROWS : 2 * ROWS] + packed[:, 2 * ROWS :]

    pl.semaphore_wait(barrier, len(everyone) + has_left.astype(jnp.int32) + has_right.astype(jnp.int32))

    def copy(source, sink, ssem, rsem, peer):
        return pltpu.make_async_remote_copy(
            src_ref=source, dst_ref=sink, send_sem=ssem, recv_sem=rsem, device_id=peer, device_id_type=MESH
        )

    def start_both(to_left, to_right):
        pl.when(has_left)(to_left.start)
        pl.when(has_right)(to_right.start)

    to_left = copy(
        mig_send.at[pl.ds(0, MOVE)], mig_recv.at[pl.ds(MOVE, MOVE)], mig_ssem.at[0], mig_rsem.at[0], left
    )
    to_right = copy(
        mig_send.at[pl.ds(MOVE, MOVE)], mig_recv.at[pl.ds(0, MOVE)], mig_ssem.at[1], mig_rsem.at[1], right
    )
    start_both(to_left, to_right)
    loads["nb"].wait()
    loads["sl"].wait()
    loads["ori"].wait()

    staying = jnp.where(target == 0, slot, -1)
    for start in range(0, CELLS, 64):
        q_ref[start : start + 64, :] = onehot(staying, 64, start)
    stay = dot_nt(x3_ref[...], q_ref[...])
    f_ref[0:ROWS, :] = stay[0:ROWS] + stay[ROWS : 2 * ROWS] + stay[2 * ROWS :]

    for side in range(2):
        for start in range(0, CELLS, 128):
            s_ref[side, start : start + 128, :] = onehot(sl_ref[side : side + 1, :], 128, start)
    mode = lax.broadcasted_iota(jnp.int32, (HALF, CELLS), 0)
    odd_first = jnp.where((mode >= 15) & (mode < 25), 2.0, 0.0)
    second = functools.reduce(jnp.logical_or, [mode == 5 * i + j for i in range(5) for j in (3, 4)])
    odd_second = jnp.where(second, 2.0, 0.0)
    outside = []
    for face in range(6):
        partner = nb_ref[face : face + 1, :]
        outside.append(jnp.where(partner < 0, 2.0, 1.0))
        for start in range(0, CELLS, 64):
            g_ref[face, start : start + 64, :] = onehot(partner, 64, start)
        if face < 2:
            for start in range(0, GHOST, 64):
                gg_ref[face, start : start + 64, :] = onehot(partner, 64, CELLS + face * GHOST + start)
        code = ori_ref[face : face + 1, :]
        first_bit = jnp.bitwise_and(code, 1).astype(F32)
        second_bit = lax.shift_right_arithmetic(code, 1).astype(F32)
        sign_ref[face] = (1.0 - odd_first * first_bit) * (1.0 - odd_second * second_bit)

    for name in ("fa", "fb", "bh", "bl", "w"):
        loads[name].wait()
    pl.when(has_left)(to_right.wait_recv)
    pl.when(has_right)(to_left.wait_recv)
    arrived = mig_recv[...].T
    place_in = arrived[BLOCK + 1 : BLOCK + 2, :].astype(jnp.int32) - 1
    for start in range(0, CELLS, 128):
        q_ref[start : start + 128, 0 : 2 * MOVE] = onehot(place_in, 128, start)
    parts = jnp.concatenate(split3(arrived), 0)
    moved = dot_nt(parts, q_ref[:, 0 : 2 * MOVE])
    field = f_ref[0:ROWS, :] + (moved[0:ROWS] + moved[ROWS : 2 * ROWS] + moved[2 * ROWS :])
    conduct = field[BLOCK : BLOCK + 1, :]
    row_ids = lax.broadcasted_iota(jnp.int32, (ROWS, CELLS), 0)
    source = jnp.where(row_ids < BLOCK, field, 0.0)
    b_ref[...] = source

    def operate(value, step):
        high, low = split2(jnp.where(row_ids == BLOCK, conduct, value))
        both = jnp.concatenate([high, low], 0)

        def forward(start, stop):
            rows = pl.ds(start, stop - start)
            f_ref[rows, :] = dot_nn(fa_ref[rows, :], both) + dot_nn(fb_ref[rows, :], high)

        def stack(face):
            high, low = split2(f_ref[face * FACE : (face + 1) * FACE, :])
            fs_ref[face, 0:FACE, :] = high
            fs_ref[face, FACE : 2 * FACE, :] = low

        def pair(product):
            return product[0:FACE] + product[FACE : 2 * FACE]

        copies = []
        forward(0, 2 * FACE)
        for side, peer in ((0, left), (1, right)):
            stack(side)
            halo_send[step, side] = pair(dot_nn(fs_ref[side], s_ref[side]))
            copies.append(
                copy(
                    halo_send.at[step, side], halo_recv.at[step, 1 - side],
                    halo_ssem.at[step, side], halo_rsem.at[step, side], peer,
                )
            )
        start_both(*copies)
        forward(2 * FACE, 6 * FACE + ROWS)
        for face in range(2, 6):
            stack(face)

        def coefficients(face, near):
            row = face * FACE
            trace = f_ref[row : row + HALF, :]
            normal = f_ref[row + HALF : row + FACE, :]
            near_conduct = near[25:26, :]
            sign = sign_ref[face]
            near_value = sign * near[0:HALF]
            near_normal = sign * near[HALF:FACE]
            penalty = PENALTY * jnp.maximum(conduct, near_conduct)
            jump = outside[face] * trace - near_value
            first = (
                penalty * jump
                - (0.5 * outside[face] * conduct) * normal
                + (0.5 * near_conduct) * near_normal
            )
            for offset, part in ((0, first), (HALF, conduct * jump)):
                high, low = split2(part)
                ch_ref[row + offset : row + offset + HALF, :] = high
                cl_ref[row + offset : row + offset + HALF, :] = low

        def backward(start, stop):
            columns = slice(start * FACE, stop * FACE)
            back_high = bh_ref[:, columns]
            return (
                dot_nn(back_high, ch_ref[columns, :])
                + dot_nn(back_high, cl_ref[columns, :])
                + dot_nn(bl_ref[:, columns], ch_ref[columns, :])
            )

        for face in range(2, 6):
            coefficients(face, pair(dot_nn(fs_ref[face ^ 1], g_ref[face])))
        local = [pair(dot_nn(fs_ref[face ^ 1], g_ref[face])) for face in range(2)]
        result = w_ref[:, 0:1] * value + conduct * f_ref[6 * FACE :, :] + backward(2, 6)
        for face in range(2):
            pl.when((has_left, has_right)[face])(copies[1 - face].wait_recv)
            high, low = split2(halo_recv[step, face])
            ghost = pair(dot_nn(jnp.concatenate([high, low], 0), gg_ref[face]))
            coefficients(face, local[face] + ghost)
        return result + backward(0, 2), copies

    image, copies_one = operate(source, 0)
    y_ref[...] = image
    second_image, copies_two = operate(image, 1)

    source = b_ref[...]
    image = y_ref[...]
    lane = lax.broadcasted_iota(jnp.int32, (1, 128), 1)
    row = jnp.zeros((1, 128), F32)
    for index, terms in enumerate(
        (source * source, source * image, image * image, source * second_image, image * second_image)
    ):
        row = row + jnp.where(lane == index, jnp.sum(terms, axis=(0, 1), keepdims=True), 0.0)

    sent = []
    for phase, (peers, landing, ssem, rsem) in enumerate(
        (
            (curve_peers, curve_recv, curve_ssem, curve_rsem),
            (x_peers, x_recv, x_ssem, x_rsem),
            (z_peers, z_recv, z_ssem, z_rsem),
        )
    ):
        row_send[phase] = row
        out = [
            copy(row_send.at[phase], landing.at[i], ssem.at[i], rsem.at[i], peer)
            for i, peer in enumerate(peers)
        ]
        for one in out:
            one.start()
        for i, one in enumerate(out):
            one.wait_recv()
            row = row + landing[i]
        sent += out

    bb, by, yy, bz, yz = (
        jnp.sum(jnp.where(lane == index, row, 0.0), axis=1, keepdims=True) for index in range(5)
    )
    alpha = bb / by
    norm_next = bb - alpha * (2.0 * by - alpha * yy)
    beta = norm_next / bb
    grow = 1.0 + beta
    curvature = grow * (grow * by - alpha * (bz + yy)) + alpha * (alpha * yz)
    alpha_next = norm_next / curvature
    first = alpha + alpha_next * grow
    second = alpha * alpha_next
    solution_out[...] = (first * source - second * image)[0:BLOCK]
    residual_out[...] = (source - first * image + second * second_image)[0:BLOCK]
    for one in sent:
        one.wait_send()
    for one_left, one_right in ((to_left, to_right), copies_one, copies_two):
        pl.when(has_left)(one_left.wait_send)
        pl.when(has_right)(one_right.wait_send)


def solution(mesh):
    n_curve, n_group = mesh.shape["curve"], mesh.shape["group"]
    x_size = min(X_SIZE, n_group)
    z_size = n_group // x_size
    constants = tables()
    call = pl.pallas_call(
        functools.partial(kernel, n_curve, n_group, x_size),
        out_shape=(pltpu.VMEM((BLOCK, CELLS), F32), pltpu.VMEM((BLOCK, CELLS), F32)),
        in_specs=[pl.BlockSpec(memory_space=pl.ANY)] * 11,
        out_specs=[pl.BlockSpec(memory_space=pltpu.VMEM)] * 2,
        scratch_shapes=[
            pltpu.VMEM((BLOCK, CELLS), F32),
            pltpu.VMEM((1, CELLS), F32),
            pltpu.VMEM((1, CELLS), jnp.int32),
            pltpu.VMEM((6, CELLS), jnp.int32),
            pltpu.VMEM((6, CELLS), jnp.int32),
            pltpu.VMEM((2, GHOST), jnp.int32),
            *[pltpu.VMEM(table.shape, table.dtype) for table in constants],
            pltpu.SemaphoreType.DMA((11,)),
            pltpu.VMEM((ROWS, CELLS), F32),
            pltpu.VMEM((ROWS, CELLS), F32),
            pltpu.VMEM((16, CELLS), F32),
            pltpu.VMEM((3 * ROWS, CELLS), BF16),
            pltpu.VMEM((CELLS, CELLS), BF16),
            pltpu.VMEM((6, CELLS, CELLS), BF16),
            pltpu.VMEM((2, GHOST, CELLS), BF16),
            pltpu.VMEM((2, CELLS, GHOST), BF16),
            pltpu.VMEM((6, HALF, CELLS), F32),
            pltpu.VMEM((6 * FACE + ROWS, CELLS), F32),
            pltpu.VMEM((6, 2 * FACE, CELLS), BF16),
            pltpu.VMEM((6 * FACE, CELLS), BF16),
            pltpu.VMEM((6 * FACE, CELLS), BF16),
            pltpu.VMEM((2 * MOVE, ROWS), F32),
            pltpu.VMEM((2 * MOVE, ROWS), F32),
            pltpu.VMEM((2, 2, FACE, GHOST), F32),
            pltpu.VMEM((2, 2, FACE, GHOST), F32),
            pltpu.VMEM((3, 1, 128), F32),
            pltpu.VMEM((n_curve - 1, 1, 128), F32),
            pltpu.VMEM((x_size - 1, 1, 128), F32),
            pltpu.VMEM((z_size - 1, 1, 128), F32),
            pltpu.SemaphoreType.DMA((2,)),
            pltpu.SemaphoreType.DMA((2,)),
            pltpu.SemaphoreType.DMA((2, 2)),
            pltpu.SemaphoreType.DMA((2, 2)),
            pltpu.SemaphoreType.DMA((n_curve - 1,)),
            pltpu.SemaphoreType.DMA((n_curve - 1,)),
            pltpu.SemaphoreType.DMA((x_size - 1,)),
            pltpu.SemaphoreType.DMA((x_size - 1,)),
            pltpu.SemaphoreType.DMA((z_size - 1,)),
            pltpu.SemaphoreType.DMA((z_size - 1,)),
        ],
        compiler_params=pltpu.CompilerParams(collective_id=0, has_side_effects=True),
    )

    def body(right_side, conductivity, destination, neighbour, orientation, send_list):
        return call(
            right_side, conductivity[None], destination[None], neighbour, orientation, send_list,
            *[jnp.asarray(table) for table in constants],
        )

    in_specs = (
        P(None, CURVE_GROUP),
        P(CURVE_GROUP),
        P(CURVE_GROUP),
        P(None, CURVE_GROUP),
        P(None, CURVE_GROUP),
        P(None, CURVE_GROUP),
    )
    out_specs = (P(None, CURVE_GROUP), P(None, CURVE_GROUP))
    return jax.shard_map(body, mesh=mesh, in_specs=in_specs, out_specs=out_specs, check_vma=False)
```

```python
import functools

import jax
import jax.numpy as jnp
import ml_dtypes
import numpy as np
from jax import lax
from jax.experimental import pallas as pl
from jax.experimental.pallas import tpu as pltpu
from jax.sharding import PartitionSpec as P

NODES = 5
BLOCK = 125
CELLS = 512
GHOST = 256
MOVE = 64
PENALTY = 80.0
FACE = 64
HALF = 32
ROWS = 128
X_SIZE = 8
MESH = pl.DeviceIdType.MESH
F32 = jnp.float32
BF16 = jnp.bfloat16
CURVE_GROUP = ("curve", "group")
GAUSS_POINTS = (-0.906179845938664, -0.5384693101056831, 0.0, 0.5384693101056831, 0.906179845938664)
GAUSS_WEIGHTS = (
    0.2369268850561891,
    0.4786286704993665,
    0.5688888888888889,
    0.4786286704993665,
    0.2369268850561891,
)


def lagrange_value(points, position, location):
    product_value = 1.0
    for other in range(len(points)):
        if other != position:
            product_value *= (location - points[other]) / (points[position] - points[other])
    return product_value


def lagrange_slope(points, position, location):
    slope_sum = 0.0
    for skipped in range(len(points)):
        if skipped == position:
            continue
        addend = 1.0 / (points[position] - points[skipped])
        for other in range(len(points)):
            if other != position and other != skipped:
                addend *= (location - points[other]) / (points[position] - points[other])
        slope_sum += addend
    return slope_sum


def along_axis(matrix, axis_id):
    eye = np.eye(NODES)
    parts = [eye, eye, eye]
    parts[axis_id] = matrix
    return np.kron(parts[0], np.kron(parts[1], parts[2]))


def tables():
    points = [0.5 * (value + 1.0) for value in GAUSS_POINTS]
    weights = np.array([0.5 * value for value in GAUSS_WEIGHTS])
    slopes = np.array([[lagrange_slope(points, p, points[q]) for p in range(NODES)] for q in range(NODES)])
    ends = [
        (
            np.array([lagrange_value(points, p, 0.0) for p in range(NODES)]),
            np.array([-lagrange_slope(points, p, 0.0) for p in range(NODES)]),
        ),
        (
            np.array([lagrange_value(points, p, 1.0) for p in range(NODES)]),
            np.array([lagrange_slope(points, p, 1.0) for p in range(NODES)]),
        ),
    ]
    cell_weight = np.kron(weights, np.kron(weights, weights))
    volume = sum(
        along_axis(slopes, a).T @ (cell_weight[:, None] * along_axis(slopes, a)) for a in range(3)
    )
    root = np.sqrt(0.5)
    modes = np.array(
        [
            [root, 0, 0, 0, root],
            [0, root, 0, root, 0],
            [0, 0, 1, 0, 0],
            [root, 0, 0, 0, -root],
            [0, root, 0, -root, 0],
        ]
    )
    modes = np.kron(modes, modes)
    mode_weight = np.array([weights[0], weights[1], weights[2], weights[0], weights[1]])
    mode_weight = np.kron(mode_weight, mode_weight)
    forward = np.zeros((6 * FACE + ROWS, ROWS))
    backward = np.zeros((ROWS, 6 * FACE))
    for face in range(6):
        trace, normal = ends[face % 2]
        trace = modes @ along_axis(trace[None, :], face // 2)
        normal = modes @ along_axis(normal[None, :], face // 2)
        row = face * FACE
        forward[row : row + 25, :BLOCK] = trace
        forward[row + 25, BLOCK] = 1.0
        forward[row + HALF : row + HALF + 25, :BLOCK] = normal
        backward[:BLOCK, row : row + 25] = trace.T * mode_weight
        backward[:BLOCK, row + HALF : row + HALF + 25] = -0.5 * normal.T * mode_weight
    forward[6 * FACE : 6 * FACE + BLOCK, :BLOCK] = volume
    weight_rows = np.zeros((ROWS, 1))
    weight_rows[:BLOCK, 0] = cell_weight

    def halves(table):
        high = table.astype(ml_dtypes.bfloat16)
        return high, (table - high.astype(np.float64)).astype(ml_dtypes.bfloat16)

    fwd_high, fwd_low = halves(forward)
    back_high, back_low = halves(backward)
    return (
        np.concatenate([fwd_high, fwd_high], 1),
        fwd_low,
        back_high,
        back_low,
        np.broadcast_to(weight_rows, (ROWS, 128)).astype(np.float32),
    )


def dot_nn(left, right):
    return jnp.dot(left, right, preferred_element_type=F32)


def dot_nt(left, right):
    return lax.dot_general(left, right, (((1,), (1,)), ((), ())), preferred_element_type=F32)


def split2(value):
    high = value.astype(BF16)
    return high, (value - high.astype(F32)).astype(BF16)


def split3(value):
    high = value.astype(BF16)
    rest = value - high.astype(F32)
    mid = rest.astype(BF16)
    return high, mid, (rest - mid.astype(F32)).astype(BF16)


def far_first(sizes):
    offsets = [tuple(int(i) for i in index) for index in np.ndindex(*sizes) if any(index)]
    offsets.sort(key=lambda index: -sum(min(i, n - i) for i, n in zip(index, sizes)))
    return [index[0] if len(sizes) == 1 else index for index in offsets]


def onehot(index_row, rows, start=0):
    ids = lax.broadcasted_iota(jnp.int32, (rows, index_row.shape[1]), 0) + start
    return jnp.where(ids == index_row, 1.0, 0.0).astype(BF16)


def kernel(
    n_curve, n_group, x_size,
    rs_hbm, cond_hbm, dest_hbm, nb_hbm, ori_hbm, sl_hbm, fa_hbm, fb_hbm, bh_hbm, bl_hbm, w_hbm,
    solution_out, residual_out,
    rs_ref, cond_ref, dest_ref, nb_ref, ori_ref, sl_ref, fa_ref, fb_ref, bh_ref, bl_ref, w_ref, load_sem,
    b_ref, y_ref, tail_ref, x3_ref, q_ref, g_ref, gg_ref, s_ref, sign_ref, f_ref, fs_ref, ch_ref, cl_ref,
    mig_send, mig_recv, halo_send, halo_recv, row_send, curve_recv, group_recv,
    mig_ssem, mig_rsem, halo_ssem, halo_rsem, curve_ssem, curve_rsem, group_ssem, group_rsem,
):
    curve = lax.axis_index("curve")
    group = lax.axis_index("group")
    me = curve * n_group + group
    total = n_curve * n_group
    has_left, has_right = me > 0, me < total - 1

    def device(rank):
        return (rank // n_group, lax.rem(rank, n_group))

    left, right = device(lax.rem(me + total - 1, total)), device(lax.rem(me + 1, total))
    z_size = n_group // x_size
    x_pos = lax.rem(group, x_size)
    z_pos = group // x_size
    curve_peers = [(lax.rem(curve + d, n_curve), group) for d in far_first((n_curve,))]
    group_peers = [
        (curve, lax.rem(z_pos + dz, z_size) * x_size + lax.rem(x_pos + dx, x_size))
        for dz, dx in far_first((z_size, x_size))
    ]
    everyone = curve_peers + group_peers

    loads = {}
    for i, (name, source, sink) in enumerate(
        (
            ("dest", dest_hbm, dest_ref),
            ("rs", rs_hbm, rs_ref),
            ("cond", cond_hbm, cond_ref),
            ("nb", nb_hbm, nb_ref),
            ("sl", sl_hbm, sl_ref),
            ("ori", ori_hbm, ori_ref),
            ("fa", fa_hbm, fa_ref),
            ("fb", fb_hbm, fb_ref),
            ("bh", bh_hbm, bh_ref),
            ("bl", bl_hbm, bl_ref),
            ("w", w_hbm, w_ref),
        )
    ):
        loads[name] = pltpu.make_async_copy(source, sink, load_sem.at[i])
        loads[name].start()
    barrier = pltpu.get_barrier_semaphore()
    for peer in everyone:
        pl.semaphore_signal(barrier, inc=1, device_id=peer, device_id_type=MESH)

    @pl.when(has_left)
    def _():
        pl.semaphore_signal(barrier, inc=1, device_id=left, device_id_type=MESH)

    @pl.when(has_right)
    def _():
        pl.semaphore_signal(barrier, inc=1, device_id=right, device_id_type=MESH)

    for start in range(0, CELLS, 64):
        ids = lax.broadcasted_iota(jnp.int32, (64, CELLS), 0) + start
        lanes = lax.broadcasted_iota(jnp.int32, (64, CELLS), 1)
        q_ref[start : start + 64, :] = jnp.where(ids <= lanes, 1.0, 0.0).astype(BF16)

    @pl.when(jnp.logical_not(has_left))
    def _():
        mig_recv[0:MOVE, :] = jnp.zeros((MOVE, ROWS), F32)
        halo_recv[:, 0] = jnp.zeros((2, FACE, GHOST), F32)

    @pl.when(jnp.logical_not(has_right))
    def _():
        mig_recv[MOVE:, :] = jnp.zeros((MOVE, ROWS), F32)
        halo_recv[:, 1] = jnp.zeros((2, FACE, GHOST), F32)

    loads["dest"].wait()

    destination = dest_ref[...]
    target = lax.shift_right_arithmetic(destination, 9) - me
    slot = jnp.bitwise_and(destination, CELLS - 1)
    row8 = lax.broadcasted_iota(jnp.int32, (8, CELLS), 0)
    leaving = jnp.where(((row8 == 0) & (target == -1)) | ((row8 == 1) & (target == 1)), 1.0, 0.0)
    counts = dot_nn(leaving.astype(BF16), q_ref[...]).astype(jnp.int32)
    place = jnp.where(target == -1, counts[0:1] - 1, jnp.where(target == 1, counts[1:2] + (MOVE - 1), -1))
    loads["rs"].wait()
    loads["cond"].wait()
    tail_ref[0:13, :] = rs_ref[112:BLOCK, :]
    tail_ref[13:14, :] = cond_ref[...]
    tail_ref[14:15, :] = (slot + 1).astype(F32)
    tail_ref[15:16, :] = jnp.zeros((1, CELLS), F32)
    for start, stop, value in ((0, 112, rs_ref[0:112, :]), (112, ROWS, tail_ref[...])):
        for i, part in enumerate(split3(value)):
            x3_ref[i * ROWS + start : i * ROWS + stop, :] = part
    packed = dot_nt(onehot(place, 2 * MOVE), x3_ref[...])
    mig_send[...] = packed[:, 0:ROWS] + packed[:, ROWS : 2 * ROWS] + packed[:, 2 * ROWS :]

    pl.semaphore_wait(barrier, len(everyone) + has_left.astype(jnp.int32) + has_right.astype(jnp.int32))

    def copy(source, sink, ssem, rsem, peer):
        return pltpu.make_async_remote_copy(
            src_ref=source, dst_ref=sink, send_sem=ssem, recv_sem=rsem, device_id=peer, device_id_type=MESH
        )

    def start_both(to_left, to_right):
        pl.when(has_left)(to_left.start)
        pl.when(has_right)(to_right.start)

    to_left = copy(
        mig_send.at[pl.ds(0, MOVE)], mig_recv.at[pl.ds(MOVE, MOVE)], mig_ssem.at[0], mig_rsem.at[0], left
    )
    to_right = copy(
        mig_send.at[pl.ds(MOVE, MOVE)], mig_recv.at[pl.ds(0, MOVE)], mig_ssem.at[1], mig_rsem.at[1], right
    )
    start_both(to_left, to_right)
    loads["nb"].wait()
    loads["sl"].wait()
    loads["ori"].wait()

    staying = jnp.where(target == 0, slot, -1)
    for start in range(0, CELLS, 64):
        q_ref[start : start + 64, :] = onehot(staying, 64, start)
    stay = dot_nt(x3_ref[...], q_ref[...])
    f_ref[0:ROWS, :] = stay[0:ROWS] + stay[ROWS : 2 * ROWS] + stay[2 * ROWS :]

    for side in range(2):
        for start in range(0, CELLS, 128):
            s_ref[side, start : start + 128, :] = onehot(sl_ref[side : side + 1, :], 128, start)
    mode = lax.broadcasted_iota(jnp.int32, (HALF, CELLS), 0)
    odd_first = jnp.where((mode >= 15) & (mode < 25), 2.0, 0.0)
    second = functools.reduce(jnp.logical_or, [mode == 5 * i + j for i in range(5) for j in (3, 4)])
    odd_second = jnp.where(second, 2.0, 0.0)
    outside = []
    for face in range(6):
        partner = nb_ref[face : face + 1, :]
        outside.append(jnp.where(partner < 0, 2.0, 1.0))
        for start in range(0, CELLS, 64):
            g_ref[face, start : start + 64, :] = onehot(partner, 64, start)
        if face < 2:
            for start in range(0, GHOST, 64):
                gg_ref[face, start : start + 64, :] = onehot(partner, 64, CELLS + face * GHOST + start)
        code = ori_ref[face : face + 1, :]
        first_bit = jnp.bitwise_and(code, 1).astype(F32)
        second_bit = lax.shift_right_arithmetic(code, 1).astype(F32)
        sign_ref[face] = (1.0 - odd_first * first_bit) * (1.0 - odd_second * second_bit)

    for name in ("fa", "fb", "bh", "bl", "w"):
        loads[name].wait()
    pl.when(has_left)(to_right.wait_recv)
    pl.when(has_right)(to_left.wait_recv)
    arrived = mig_recv[...].T
    place_in = arrived[BLOCK + 1 : BLOCK + 2, :].astype(jnp.int32) - 1
    for start in range(0, CELLS, 128):
        q_ref[start : start + 128, 0 : 2 * MOVE] = onehot(place_in, 128, start)
    parts = jnp.concatenate(split3(arrived), 0)
    moved = dot_nt(parts, q_ref[:, 0 : 2 * MOVE])
    field = f_ref[0:ROWS, :] + (moved[0:ROWS] + moved[ROWS : 2 * ROWS] + moved[2 * ROWS :])
    conduct = field[BLOCK : BLOCK + 1, :]
    row_ids = lax.broadcasted_iota(jnp.int32, (ROWS, CELLS), 0)
    source = jnp.where(row_ids < BLOCK, field, 0.0)
    b_ref[...] = source

    def operate(value, step):
        high, low = split2(jnp.where(row_ids == BLOCK, conduct, value))
        both = jnp.concatenate([high, low], 0)

        def forward(start, stop):
            rows = pl.ds(start, stop - start)
            f_ref[rows, :] = dot_nn(fa_ref[rows, :], both) + dot_nn(fb_ref[rows, :], high)

        def stack(face):
            high, low = split2(f_ref[face * FACE : (face + 1) * FACE, :])
            fs_ref[face, 0:FACE, :] = high
            fs_ref[face, FACE : 2 * FACE, :] = low

        def pair(product):
            return product[0:FACE] + product[FACE : 2 * FACE]

        copies = []
        forward(0, 2 * FACE)
        for side, peer in ((0, left), (1, right)):
            stack(side)
            halo_send[step, side] = pair(dot_nn(fs_ref[side], s_ref[side]))
            copies.append(
                copy(
                    halo_send.at[step, side], halo_recv.at[step, 1 - side],
                    halo_ssem.at[step, side], halo_rsem.at[step, side], peer,
                )
            )
        start_both(*copies)
        forward(2 * FACE, 6 * FACE + ROWS)
        for face in range(2, 6):
            stack(face)

        def coefficients(face, near):
            row = face * FACE
            trace = f_ref[row : row + HALF, :]
            normal = f_ref[row + HALF : row + FACE, :]
            near_conduct = near[25:26, :]
            sign = sign_ref[face]
            near_value = sign * near[0:HALF]
            near_normal = sign * near[HALF:FACE]
            penalty = PENALTY * jnp.maximum(conduct, near_conduct)
            jump = outside[face] * trace - near_value
            first = (
                penalty * jump
                - (0.5 * outside[face] * conduct) * normal
                + (0.5 * near_conduct) * near_normal
            )
            for offset, part in ((0, first), (HALF, conduct * jump)):
                high, low = split2(part)
                ch_ref[row + offset : row + offset + HALF, :] = high
                cl_ref[row + offset : row + offset + HALF, :] = low

        def backward(start, stop):
            columns = slice(start * FACE, stop * FACE)
            back_high = bh_ref[:, columns]
            return (
                dot_nn(back_high, ch_ref[columns, :])
                + dot_nn(back_high, cl_ref[columns, :])
                + dot_nn(bl_ref[:, columns], ch_ref[columns, :])
            )

        for face in range(2, 6):
            coefficients(face, pair(dot_nn(fs_ref[face ^ 1], g_ref[face])))
        local = [pair(dot_nn(fs_ref[face ^ 1], g_ref[face])) for face in range(2)]
        result = w_ref[:, 0:1] * value + conduct * f_ref[6 * FACE :, :] + backward(2, 6)
        for face in range(2):
            pl.when((has_left, has_right)[face])(copies[1 - face].wait_recv)
            high, low = split2(halo_recv[step, face])
            ghost = pair(dot_nn(jnp.concatenate([high, low], 0), gg_ref[face]))
            coefficients(face, local[face] + ghost)
        return result + backward(0, 2), copies

    image, copies_one = operate(source, 0)
    y_ref[...] = image
    second_image, copies_two = operate(image, 1)

    source = b_ref[...]
    image = y_ref[...]
    lane = lax.broadcasted_iota(jnp.int32, (1, 128), 1)
    row = jnp.zeros((1, 128), F32)
    for index, terms in enumerate(
        (source * source, source * image, image * image, source * second_image, image * second_image)
    ):
        row = row + jnp.where(lane == index, jnp.sum(terms, axis=(0, 1), keepdims=True), 0.0)

    sent = []
    for phase, (peers, landing, ssem, rsem) in enumerate(
        (
            (curve_peers, curve_recv, curve_ssem, curve_rsem),
            (group_peers, group_recv, group_ssem, group_rsem),
        )
    ):
        row_send[phase] = row
        out = [
            copy(row_send.at[phase], landing.at[i], ssem.at[i], rsem.at[i], peer)
            for i, peer in enumerate(peers)
        ]
        for one in out:
            one.start()
        for one in out:
            one.wait_recv()
        terms = [row] + [landing[i] for i in range(len(out))]
        while len(terms) > 1:
            terms = [sum(terms[i + 1 : i + 2], terms[i]) for i in range(0, len(terms), 2)]
        row = terms[0]
        sent += out

    bb, by, yy, bz, yz = (
        jnp.sum(jnp.where(lane == index, row, 0.0), axis=1, keepdims=True) for index in range(5)
    )
    alpha = bb / by
    norm_next = bb - alpha * (2.0 * by - alpha * yy)
    beta = norm_next / bb
    grow = 1.0 + beta
    curvature = grow * (grow * by - alpha * (bz + yy)) + alpha * (alpha * yz)
    alpha_next = norm_next / curvature
    first = alpha + alpha_next * grow
    second = alpha * alpha_next
    solution_out[...] = (first * source - second * image)[0:BLOCK]
    residual_out[...] = (source - first * image + second * second_image)[0:BLOCK]
    for one in sent:
        one.wait_send()
    for one_left, one_right in ((to_left, to_right), copies_one, copies_two):
        pl.when(has_left)(one_left.wait_send)
        pl.when(has_right)(one_right.wait_send)


def write_kernel(solution_ref, residual_ref, solution_out, residual_out, sem):
    copies = [
        pltpu.make_async_copy(solution_ref, solution_out, sem.at[0]),
        pltpu.make_async_copy(residual_ref, residual_out, sem.at[1]),
    ]
    for one in copies:
        one.start()
    for one in copies:
        one.wait()


def solution(mesh):
    n_curve, n_group = mesh.shape["curve"], mesh.shape["group"]
    x_size = min(X_SIZE, n_group)
    constants = tables()
    call = pl.pallas_call(
        functools.partial(kernel, n_curve, n_group, x_size),
        out_shape=(pltpu.VMEM((BLOCK, CELLS), F32), pltpu.VMEM((BLOCK, CELLS), F32)),
        in_specs=[pl.BlockSpec(memory_space=pl.ANY)] * 11,
        out_specs=[pl.BlockSpec(memory_space=pltpu.VMEM)] * 2,
        scratch_shapes=[
            pltpu.VMEM((BLOCK, CELLS), F32),
            pltpu.VMEM((1, CELLS), F32),
            pltpu.VMEM((1, CELLS), jnp.int32),
            pltpu.VMEM((6, CELLS), jnp.int32),
            pltpu.VMEM((6, CELLS), jnp.int32),
            pltpu.VMEM((2, GHOST), jnp.int32),
            *[pltpu.VMEM(table.shape, table.dtype) for table in constants],
            pltpu.SemaphoreType.DMA((11,)),
            pltpu.VMEM((ROWS, CELLS), F32),
            pltpu.VMEM((ROWS, CELLS), F32),
            pltpu.VMEM((16, CELLS), F32),
            pltpu.VMEM((3 * ROWS, CELLS), BF16),
            pltpu.VMEM((CELLS, CELLS), BF16),
            pltpu.VMEM((6, CELLS, CELLS), BF16),
            pltpu.VMEM((2, GHOST, CELLS), BF16),
            pltpu.VMEM((2, CELLS, GHOST), BF16),
            pltpu.VMEM((6, HALF, CELLS), F32),
            pltpu.VMEM((6 * FACE + ROWS, CELLS), F32),
            pltpu.VMEM((6, 2 * FACE, CELLS), BF16),
            pltpu.VMEM((6 * FACE, CELLS), BF16),
            pltpu.VMEM((6 * FACE, CELLS), BF16),
            pltpu.VMEM((2 * MOVE, ROWS), F32),
            pltpu.VMEM((2 * MOVE, ROWS), F32),
            pltpu.VMEM((2, 2, FACE, GHOST), F32),
            pltpu.VMEM((2, 2, FACE, GHOST), F32),
            pltpu.VMEM((2, 1, 128), F32),
            pltpu.VMEM((n_curve - 1, 1, 128), F32),
            pltpu.VMEM((n_group - 1, 1, 128), F32),
            pltpu.SemaphoreType.DMA((2,)),
            pltpu.SemaphoreType.DMA((2,)),
            pltpu.SemaphoreType.DMA((2, 2)),
            pltpu.SemaphoreType.DMA((2, 2)),
            pltpu.SemaphoreType.DMA((n_curve - 1,)),
            pltpu.SemaphoreType.DMA((n_curve - 1,)),
            pltpu.SemaphoreType.DMA((n_group - 1,)),
            pltpu.SemaphoreType.DMA((n_group - 1,)),
        ],
        compiler_params=pltpu.CompilerParams(collective_id=0, has_side_effects=True),
    )

    field = jax.ShapeDtypeStruct((BLOCK, CELLS), F32)
    write = pl.pallas_call(
        write_kernel,
        out_shape=(field, field),
        in_specs=[pl.BlockSpec(memory_space=pltpu.VMEM)] * 2,
        out_specs=[pl.BlockSpec(memory_space=pl.ANY)] * 2,
        scratch_shapes=[pltpu.SemaphoreType.DMA((2,))],
    )

    def body(right_side, conductivity, destination, neighbour, orientation, send_list):
        fields = call(
            right_side, conductivity[None], destination[None], neighbour, orientation, send_list,
            *[jnp.asarray(table) for table in constants],
        )
        return write(*[pltpu.with_memory_space_constraint(one, pltpu.VMEM) for one in fields])

    in_specs = (
        P(None, CURVE_GROUP),
        P(CURVE_GROUP),
        P(CURVE_GROUP),
        P(None, CURVE_GROUP),
        P(None, CURVE_GROUP),
        P(None, CURVE_GROUP),
    )
    out_specs = (P(None, CURVE_GROUP), P(None, CURVE_GROUP))
    return jax.shard_map(body, mesh=mesh, in_specs=in_specs, out_specs=out_specs, check_vma=False)
```

```python
import functools

import jax
import jax.numpy as jnp
import ml_dtypes
import numpy as np
from jax import lax
from jax.experimental import pallas as pl
from jax.experimental.pallas import tpu as pltpu
from jax.sharding import PartitionSpec as P

NODES = 5
BLOCK = 125
CELLS = 512
GHOST = 256
MOVE = 64
PENALTY = 80.0
FACE = 64
HALF = 32
ROWS = 128
X_SIZE = 8
MESH = pl.DeviceIdType.MESH
F32 = jnp.float32
BF16 = jnp.bfloat16
CURVE_GROUP = ("curve", "group")
GAUSS_POINTS = (-0.906179845938664, -0.5384693101056831, 0.0, 0.5384693101056831, 0.906179845938664)
GAUSS_WEIGHTS = (
    0.2369268850561891,
    0.4786286704993665,
    0.5688888888888889,
    0.4786286704993665,
    0.2369268850561891,
)


def lagrange_value(points, position, location):
    product_value = 1.0
    for other in range(len(points)):
        if other != position:
            product_value *= (location - points[other]) / (points[position] - points[other])
    return product_value


def lagrange_slope(points, position, location):
    slope_sum = 0.0
    for skipped in range(len(points)):
        if skipped == position:
            continue
        addend = 1.0 / (points[position] - points[skipped])
        for other in range(len(points)):
            if other != position and other != skipped:
                addend *= (location - points[other]) / (points[position] - points[other])
        slope_sum += addend
    return slope_sum


def along_axis(matrix, axis_id):
    eye = np.eye(NODES)
    parts = [eye, eye, eye]
    parts[axis_id] = matrix
    return np.kron(parts[0], np.kron(parts[1], parts[2]))


def tables():
    points = [0.5 * (value + 1.0) for value in GAUSS_POINTS]
    weights = np.array([0.5 * value for value in GAUSS_WEIGHTS])
    slopes = np.array([[lagrange_slope(points, p, points[q]) for p in range(NODES)] for q in range(NODES)])
    ends = [
        (
            np.array([lagrange_value(points, p, 0.0) for p in range(NODES)]),
            np.array([-lagrange_slope(points, p, 0.0) for p in range(NODES)]),
        ),
        (
            np.array([lagrange_value(points, p, 1.0) for p in range(NODES)]),
            np.array([lagrange_slope(points, p, 1.0) for p in range(NODES)]),
        ),
    ]
    cell_weight = np.kron(weights, np.kron(weights, weights))
    volume = sum(
        along_axis(slopes, a).T @ (cell_weight[:, None] * along_axis(slopes, a)) for a in range(3)
    )
    root = np.sqrt(0.5)
    modes = np.array(
        [
            [root, 0, 0, 0, root],
            [0, root, 0, root, 0],
            [0, 0, 1, 0, 0],
            [root, 0, 0, 0, -root],
            [0, root, 0, -root, 0],
        ]
    )
    modes = np.kron(modes, modes)
    mode_weight = np.array([weights[0], weights[1], weights[2], weights[0], weights[1]])
    mode_weight = np.kron(mode_weight, mode_weight)
    forward = np.zeros((6 * FACE + ROWS, ROWS))
    backward = np.zeros((ROWS, 6 * FACE))
    for face in range(6):
        trace, normal = ends[face % 2]
        trace = modes @ along_axis(trace[None, :], face // 2)
        normal = modes @ along_axis(normal[None, :], face // 2)
        row = face * FACE
        forward[row : row + 25, :BLOCK] = trace
        forward[row + 25, BLOCK] = 1.0
        forward[row + HALF : row + HALF + 25, :BLOCK] = normal
        backward[:BLOCK, row : row + 25] = trace.T * mode_weight
        backward[:BLOCK, row + HALF : row + HALF + 25] = -0.5 * normal.T * mode_weight
    forward[6 * FACE : 6 * FACE + BLOCK, :BLOCK] = volume
    weight_rows = np.zeros((ROWS, 1))
    weight_rows[:BLOCK, 0] = cell_weight

    def halves(table):
        high = table.astype(ml_dtypes.bfloat16)
        return high, (table - high.astype(np.float64)).astype(ml_dtypes.bfloat16)

    fwd_high, fwd_low = halves(forward)
    back_high, back_low = halves(backward)
    return (
        np.concatenate([np.concatenate([fwd_high, fwd_high, fwd_low], 1), back_high, back_low], 0),
        np.broadcast_to(weight_rows, (ROWS, 128)).astype(np.float32),
    )


def dot_nn(left, right):
    return jnp.dot(left, right, preferred_element_type=F32)


def dot_nt(left, right):
    return lax.dot_general(left, right, (((1,), (1,)), ((), ())), preferred_element_type=F32)


def split2(value):
    high = value.astype(BF16)
    return high, (value - high.astype(F32)).astype(BF16)


def split3(value):
    high = value.astype(BF16)
    rest = value - high.astype(F32)
    mid = rest.astype(BF16)
    return high, mid, (rest - mid.astype(F32)).astype(BF16)


def far_first(sizes):
    offsets = [tuple(int(i) for i in index) for index in np.ndindex(*sizes) if any(index)]
    offsets.sort(key=lambda index: -sum(min(i, n - i) for i, n in zip(index, sizes)))
    return [index[0] if len(sizes) == 1 else index for index in offsets]


def onehot(index_row, rows, start=0):
    ids = lax.broadcasted_iota(jnp.int32, (rows, index_row.shape[1]), 0) + start
    return jnp.where(ids == index_row, 1.0, 0.0).astype(BF16)


def kernel(
    n_curve, n_group, x_size,
    rs_hbm, cond_hbm, dest_hbm, nb_hbm, ori_hbm, sl_hbm, table_hbm, w_hbm,
    solution_out, residual_out,
    rs_ref, cond_ref, dest_ref, nb_ref, ori_ref, sl_ref, table_ref, w_ref, load_sem,
    b_ref, y_ref, tail_ref, x3_ref, q_ref, g_ref, gg_ref, s_ref, sign_ref, f_ref, fs_ref, ch_ref, cl_ref,
    mig_send, mig_recv, halo_send, halo_recv, row_send, curve_recv, group_recv,
    mig_ssem, mig_rsem, halo_ssem, halo_rsem, curve_ssem, curve_rsem, group_ssem, group_rsem, one_sem, two_sem, plane_sem,
):
    curve = lax.axis_index("curve")
    group = lax.axis_index("group")
    me = curve * n_group + group
    total = n_curve * n_group
    has_left, has_right = me > 0, me < total - 1

    def device(rank):
        return (rank // n_group, lax.rem(rank, n_group))

    left, right = device(lax.rem(me + total - 1, total)), device(lax.rem(me + 1, total))
    z_size = n_group // x_size
    x_pos = lax.rem(group, x_size)
    z_pos = group // x_size
    curve_peers = [(lax.rem(curve + d, n_curve), group) for d in far_first((n_curve,))]
    group_peers = [
        (curve, lax.rem(z_pos + dz, z_size) * x_size + lax.rem(x_pos + dx, x_size))
        for dz, dx in far_first((z_size, x_size))
    ]
    y_size = n_curve // 2
    core = lax.rem(curve, 2)
    core_peer = (curve + 1 - 2 * core, group)

    def along(dim, offset):
        if dim == 0:
            return (curve, z_pos * x_size + lax.rem(x_pos + offset, x_size))
        if dim == 1:
            return (lax.rem(curve + 2 * offset, n_curve), group)
        return (curve, lax.rem(z_pos + offset, z_size) * x_size + x_pos)

    sizes = (x_size, y_size, z_size)
    near_peers = [core_peer] + [
        along(dim, offset) for dim in range(3) for offset in sorted({1, sizes[dim] - 1}) if sizes[dim] > 1
    ]

    def signal(sem, peer):
        pl.semaphore_signal(sem, inc=1, device_id=peer, device_id_type=MESH)

    def spread(reach, ring_sem):
        for dim in range(3):
            if sizes[dim] > 2 * reach + 1:
                signal(ring_sem.at[dim], along(dim, reach))
                signal(ring_sem.at[dim], along(dim, sizes[dim] - reach))

    def gather_known(reach, ring_sem):
        for dim in range(3):
            if sizes[dim] > 2 * reach + 1:
                pl.semaphore_wait(ring_sem.at[dim], 2)

    def after_moves():
        gather_known(1, one_sem)
        spread(2, two_sem)

    def after_first():
        gather_known(2, two_sem)
        signal(plane_sem.at[0], core_peer)
        for offset in range(1, x_size):
            signal(plane_sem.at[1], along(0, offset))

    def before_sums():
        pl.semaphore_wait(plane_sem.at[0], 1)
        if x_size > 1:
            pl.semaphore_wait(plane_sem.at[1], x_size - 1)

    loads = {}
    for i, (name, source, sink) in enumerate(
        (
            ("dest", dest_hbm, dest_ref),
            ("rs", rs_hbm, rs_ref),
            ("cond", cond_hbm, cond_ref),
            ("nb", nb_hbm, nb_ref),
            ("sl", sl_hbm, sl_ref),
            ("ori", ori_hbm, ori_ref),
            ("table", table_hbm, table_ref),
            ("w", w_hbm, w_ref),
        )
    ):
        loads[name] = pltpu.make_async_copy(source, sink, load_sem.at[i])
        loads[name].start()
    barrier = pltpu.get_barrier_semaphore()
    for peer in near_peers:
        signal(barrier, peer)

    @pl.when(has_left)
    def _():
        signal(barrier, left)

    @pl.when(has_right)
    def _():
        signal(barrier, right)

    for start in range(0, CELLS, 64):
        ids = lax.broadcasted_iota(jnp.int32, (64, CELLS), 0) + start
        lanes = lax.broadcasted_iota(jnp.int32, (64, CELLS), 1)
        q_ref[start : start + 64, :] = jnp.where(ids <= lanes, 1.0, 0.0).astype(BF16)

    @pl.when(jnp.logical_not(has_left))
    def _():
        mig_recv[0:MOVE, :] = jnp.zeros((MOVE, ROWS), F32)
        halo_recv[:, 0] = jnp.zeros((2, FACE, GHOST), F32)

    @pl.when(jnp.logical_not(has_right))
    def _():
        mig_recv[MOVE:, :] = jnp.zeros((MOVE, ROWS), F32)
        halo_recv[:, 1] = jnp.zeros((2, FACE, GHOST), F32)

    loads["dest"].wait()

    destination = dest_ref[...]
    target = lax.shift_right_arithmetic(destination, 9) - me
    slot = jnp.bitwise_and(destination, CELLS - 1)
    row8 = lax.broadcasted_iota(jnp.int32, (8, CELLS), 0)
    leaving = jnp.where(((row8 == 0) & (target == -1)) | ((row8 == 1) & (target == 1)), 1.0, 0.0)
    counts = dot_nn(leaving.astype(BF16), q_ref[...]).astype(jnp.int32)
    place = jnp.where(target == -1, counts[0:1] - 1, jnp.where(target == 1, counts[1:2] + (MOVE - 1), -1))
    loads["rs"].wait()
    loads["cond"].wait()
    tail_ref[0:13, :] = rs_ref[112:BLOCK, :]
    tail_ref[13:14, :] = cond_ref[...]
    tail_ref[14:15, :] = (slot + 1).astype(F32)
    tail_ref[15:16, :] = jnp.zeros((1, CELLS), F32)
    for start, stop, value in ((0, 112, rs_ref[0:112, :]), (112, ROWS, tail_ref[...])):
        for i, part in enumerate(split3(value)):
            x3_ref[i * ROWS + start : i * ROWS + stop, :] = part
    packed = dot_nt(onehot(place, 2 * MOVE), x3_ref[...])
    mig_send[...] = packed[:, 0:ROWS] + packed[:, ROWS : 2 * ROWS] + packed[:, 2 * ROWS :]

    pl.semaphore_wait(barrier, len(near_peers) + has_left.astype(jnp.int32) + has_right.astype(jnp.int32))

    def copy(source, sink, ssem, rsem, peer):
        return pltpu.make_async_remote_copy(
            src_ref=source, dst_ref=sink, send_sem=ssem, recv_sem=rsem, device_id=peer, device_id_type=MESH
        )

    def start_both(to_left, to_right):
        pl.when(has_left)(to_left.start)
        pl.when(has_right)(to_right.start)

    to_left = copy(
        mig_send.at[pl.ds(0, MOVE)], mig_recv.at[pl.ds(MOVE, MOVE)], mig_ssem.at[0], mig_rsem.at[0], left
    )
    to_right = copy(
        mig_send.at[pl.ds(MOVE, MOVE)], mig_recv.at[pl.ds(0, MOVE)], mig_ssem.at[1], mig_rsem.at[1], right
    )
    start_both(to_left, to_right)
    spread(1, one_sem)
    loads["nb"].wait()
    loads["sl"].wait()
    loads["ori"].wait()

    staying = jnp.where(target == 0, slot, -1)
    for start in range(0, CELLS, 64):
        q_ref[start : start + 64, :] = onehot(staying, 64, start)
    stay = dot_nt(x3_ref[...], q_ref[...])
    f_ref[0:ROWS, :] = stay[0:ROWS] + stay[ROWS : 2 * ROWS] + stay[2 * ROWS :]

    for side in range(2):
        for start in range(0, CELLS, 128):
            s_ref[side, start : start + 128, :] = onehot(sl_ref[side : side + 1, :], 128, start)
    mode = lax.broadcasted_iota(jnp.int32, (HALF, CELLS), 0)
    odd_first = jnp.where((mode >= 15) & (mode < 25), 2.0, 0.0)
    second = functools.reduce(jnp.logical_or, [mode == 5 * i + j for i in range(5) for j in (3, 4)])
    odd_second = jnp.where(second, 2.0, 0.0)
    outside = []
    for face in range(6):
        partner = nb_ref[face : face + 1, :]
        outside.append(jnp.where(partner < 0, 2.0, 1.0))
        for start in range(0, CELLS, 64):
            g_ref[face, start : start + 64, :] = onehot(partner, 64, start)
        if face < 2:
            for start in range(0, GHOST, 64):
                gg_ref[face, start : start + 64, :] = onehot(partner, 64, CELLS + face * GHOST + start)
        code = ori_ref[face : face + 1, :]
        first_bit = jnp.bitwise_and(code, 1).astype(F32)
        second_bit = lax.shift_right_arithmetic(code, 1).astype(F32)
        sign_ref[face] = (1.0 - odd_first * first_bit) * (1.0 - odd_second * second_bit)

    loads["table"].wait()
    loads["w"].wait()
    pl.when(has_left)(to_right.wait_recv)
    pl.when(has_right)(to_left.wait_recv)
    arrived = mig_recv[...].T
    place_in = arrived[BLOCK + 1 : BLOCK + 2, :].astype(jnp.int32) - 1
    for start in range(0, CELLS, 128):
        q_ref[start : start + 128, 0 : 2 * MOVE] = onehot(place_in, 128, start)
    parts = jnp.concatenate(split3(arrived), 0)
    moved = dot_nt(parts, q_ref[:, 0 : 2 * MOVE])
    field = f_ref[0:ROWS, :] + (moved[0:ROWS] + moved[ROWS : 2 * ROWS] + moved[2 * ROWS :])
    conduct = field[BLOCK : BLOCK + 1, :]
    row_ids = lax.broadcasted_iota(jnp.int32, (ROWS, CELLS), 0)
    source = jnp.where(row_ids < BLOCK, field, 0.0)
    b_ref[...] = source

    def operate(value, step):
        high, low = split2(jnp.where(row_ids == BLOCK, conduct, value))
        both = jnp.concatenate([high, low], 0)

        def forward(start, stop):
            rows = pl.ds(start, stop - start)
            f_ref[rows, :] = dot_nn(table_ref[rows, 0:256], both) + dot_nn(table_ref[rows, 256:384], high)

        def stack(face):
            high, low = split2(f_ref[face * FACE : (face + 1) * FACE, :])
            fs_ref[face, 0:FACE, :] = high
            fs_ref[face, FACE : 2 * FACE, :] = low

        def pair(product):
            return product[0:FACE] + product[FACE : 2 * FACE]

        copies = []
        forward(0, 2 * FACE)
        for side, peer in ((0, left), (1, right)):
            stack(side)
            halo_send[step, side] = pair(dot_nn(fs_ref[side], s_ref[side]))
            copies.append(
                copy(
                    halo_send.at[step, side], halo_recv.at[step, 1 - side],
                    halo_ssem.at[step, side], halo_rsem.at[step, side], peer,
                )
            )
        start_both(*copies)
        forward(2 * FACE, 6 * FACE + ROWS)
        for face in range(2, 6):
            stack(face)

        def coefficients(face, near):
            row = face * FACE
            trace = f_ref[row : row + HALF, :]
            normal = f_ref[row + HALF : row + FACE, :]
            near_conduct = near[25:26, :]
            sign = sign_ref[face]
            near_value = sign * near[0:HALF]
            near_normal = sign * near[HALF:FACE]
            penalty = PENALTY * jnp.maximum(conduct, near_conduct)
            jump = outside[face] * trace - near_value
            first = (
                penalty * jump
                - (0.5 * outside[face] * conduct) * normal
                + (0.5 * near_conduct) * near_normal
            )
            for offset, part in ((0, first), (HALF, conduct * jump)):
                high, low = split2(part)
                ch_ref[row + offset : row + offset + HALF, :] = high
                cl_ref[row + offset : row + offset + HALF, :] = low

        def backward(start, stop):
            columns = slice(start * FACE, stop * FACE)
            back_high = table_ref[512:640, columns]
            return (
                dot_nn(back_high, ch_ref[columns, :])
                + dot_nn(back_high, cl_ref[columns, :])
                + dot_nn(table_ref[640:768, columns], ch_ref[columns, :])
            )

        for face in range(2, 6):
            coefficients(face, pair(dot_nn(fs_ref[face ^ 1], g_ref[face])))
        local = [pair(dot_nn(fs_ref[face ^ 1], g_ref[face])) for face in range(2)]
        result = w_ref[:, 0:1] * value + conduct * f_ref[6 * FACE :, :] + backward(2, 6)
        (after_moves, after_first)[step]()
        for face in range(2):
            pl.when((has_left, has_right)[face])(copies[1 - face].wait_recv)
            high, low = split2(halo_recv[step, face])
            ghost = pair(dot_nn(jnp.concatenate([high, low], 0), gg_ref[face]))
            coefficients(face, local[face] + ghost)
        return result + backward(0, 2), copies

    image, copies_one = operate(source, 0)
    y_ref[...] = image
    second_image, copies_two = operate(image, 1)

    source = b_ref[...]
    image = y_ref[...]
    lane = lax.broadcasted_iota(jnp.int32, (1, 128), 1)
    row = jnp.zeros((1, 128), F32)
    for index, terms in enumerate(
        (source * source, source * image, image * image, source * second_image, image * second_image)
    ):
        row = row + jnp.where(lane == index, jnp.sum(terms, axis=(0, 1), keepdims=True), 0.0)

    before_sums()
    sent = []
    for phase, (peers, landing, ssem, rsem) in enumerate(
        (
            (curve_peers, curve_recv, curve_ssem, curve_rsem),
            (group_peers, group_recv, group_ssem, group_rsem),
        )
    ):
        row_send[phase] = row
        for i, peer in enumerate(peers):
            copy(row_send.at[phase], landing.at[i], ssem, rsem, peer).start()
        every = copy(landing, landing, ssem, rsem, peers[0])
        every.wait_recv()
        terms = [row] + [landing[i] for i in range(len(peers))]
        while len(terms) > 1:
            terms = [sum(terms[i + 1 : i + 2], terms[i]) for i in range(0, len(terms), 2)]
        row = terms[0]
        sent.append(every)

    bb, by, yy, bz, yz = (
        jnp.sum(jnp.where(lane == index, row, 0.0), axis=1, keepdims=True) for index in range(5)
    )
    alpha = bb / by
    norm_next = bb - alpha * (2.0 * by - alpha * yy)
    beta = norm_next / bb
    grow = 1.0 + beta
    curvature = grow * (grow * by - alpha * (bz + yy)) + alpha * (alpha * yz)
    alpha_next = norm_next / curvature
    first = alpha + alpha_next * grow
    second = alpha * alpha_next
    solution_out[...] = (first * source - second * image)[0:BLOCK]
    residual_out[...] = (source - first * image + second * second_image)[0:BLOCK]
    for one in sent:
        one.wait_send()
    for one_left, one_right in ((to_left, to_right), copies_one, copies_two):
        pl.when(has_left)(one_left.wait_send)
        pl.when(has_right)(one_right.wait_send)


def write_kernel(solution_ref, residual_ref, solution_out, residual_out, sem):
    copies = [
        pltpu.make_async_copy(solution_ref, solution_out, sem.at[0]),
        pltpu.make_async_copy(residual_ref, residual_out, sem.at[1]),
    ]
    for one in copies:
        one.start()
    for one in copies:
        one.wait()


def solution(mesh):
    n_curve, n_group = mesh.shape["curve"], mesh.shape["group"]
    x_size = min(X_SIZE, n_group)
    constants = tables()
    call = pl.pallas_call(
        functools.partial(kernel, n_curve, n_group, x_size),
        out_shape=(pltpu.VMEM((BLOCK, CELLS), F32), pltpu.VMEM((BLOCK, CELLS), F32)),
        in_specs=[pl.BlockSpec(memory_space=pl.ANY)] * 8,
        out_specs=[pl.BlockSpec(memory_space=pltpu.VMEM)] * 2,
        scratch_shapes=[
            pltpu.VMEM((BLOCK, CELLS), F32),
            pltpu.VMEM((1, CELLS), F32),
            pltpu.VMEM((1, CELLS), jnp.int32),
            pltpu.VMEM((6, CELLS), jnp.int32),
            pltpu.VMEM((6, CELLS), jnp.int32),
            pltpu.VMEM((2, GHOST), jnp.int32),
            *[pltpu.VMEM(table.shape, table.dtype) for table in constants],
            pltpu.SemaphoreType.DMA((8,)),
            pltpu.VMEM((ROWS, CELLS), F32),
            pltpu.VMEM((ROWS, CELLS), F32),
            pltpu.VMEM((16, CELLS), F32),
            pltpu.VMEM((3 * ROWS, CELLS), BF16),
            pltpu.VMEM((CELLS, CELLS), BF16),
            pltpu.VMEM((6, CELLS, CELLS), BF16),
            pltpu.VMEM((2, GHOST, CELLS), BF16),
            pltpu.VMEM((2, CELLS, GHOST), BF16),
            pltpu.VMEM((6, HALF, CELLS), F32),
            pltpu.VMEM((6 * FACE + ROWS, CELLS), F32),
            pltpu.VMEM((6, 2 * FACE, CELLS), BF16),
            pltpu.VMEM((6 * FACE, CELLS), BF16),
            pltpu.VMEM((6 * FACE, CELLS), BF16),
            pltpu.VMEM((2 * MOVE, ROWS), F32),
            pltpu.VMEM((2 * MOVE, ROWS), F32),
            pltpu.VMEM((2, 2, FACE, GHOST), F32),
            pltpu.VMEM((2, 2, FACE, GHOST), F32),
            pltpu.VMEM((2, 1, 128), F32),
            pltpu.VMEM((n_curve - 1, 1, 128), F32),
            pltpu.VMEM((n_group - 1, 1, 128), F32),
            pltpu.SemaphoreType.DMA((2,)),
            pltpu.SemaphoreType.DMA((2,)),
            pltpu.SemaphoreType.DMA((2, 2)),
            pltpu.SemaphoreType.DMA((2, 2)),
            pltpu.SemaphoreType.DMA,
            pltpu.SemaphoreType.DMA,
            pltpu.SemaphoreType.DMA,
            pltpu.SemaphoreType.DMA,
            pltpu.SemaphoreType.REGULAR((3,)),
            pltpu.SemaphoreType.REGULAR((3,)),
            pltpu.SemaphoreType.REGULAR((2,)),
        ],
        compiler_params=pltpu.CompilerParams(collective_id=0, has_side_effects=True),
    )

    field = jax.ShapeDtypeStruct((BLOCK, CELLS), F32)
    write = pl.pallas_call(
        write_kernel,
        out_shape=(field, field),
        in_specs=[pl.BlockSpec(memory_space=pltpu.VMEM)] * 2,
        out_specs=[pl.BlockSpec(memory_space=pl.ANY)] * 2,
        scratch_shapes=[pltpu.SemaphoreType.DMA((2,))],
    )

    def body(right_side, conductivity, destination, neighbour, orientation, send_list):
        fields = call(
            right_side, conductivity[None], destination[None], neighbour, orientation, send_list,
            *[jnp.asarray(table) for table in constants],
        )
        return write(*[pltpu.with_memory_space_constraint(one, pltpu.VMEM) for one in fields])

    in_specs = (
        P(None, CURVE_GROUP),
        P(CURVE_GROUP),
        P(CURVE_GROUP),
        P(None, CURVE_GROUP),
        P(None, CURVE_GROUP),
        P(None, CURVE_GROUP),
    )
    out_specs = (P(None, CURVE_GROUP), P(None, CURVE_GROUP))
    return jax.shard_map(body, mesh=mesh, in_specs=in_specs, out_specs=out_specs, check_vma=False)
```

```python
import functools

import jax
import jax.numpy as jnp
import ml_dtypes
import numpy as np
from jax import lax
from jax.experimental import pallas as pl
from jax.experimental.pallas import tpu as pltpu
from jax.sharding import PartitionSpec as P

NODES = 5
BLOCK = 125
CELLS = 512
GHOST = 256
MOVE = 64
PENALTY = 80.0
FACE = 64
HALF = 32
ROWS = 128
X_SIZE = 8
MESH = pl.DeviceIdType.MESH
F32 = jnp.float32
BF16 = jnp.bfloat16
CURVE_GROUP = ("curve", "group")
GAUSS_POINTS = (-0.906179845938664, -0.5384693101056831, 0.0, 0.5384693101056831, 0.906179845938664)
GAUSS_WEIGHTS = (
    0.2369268850561891,
    0.4786286704993665,
    0.5688888888888889,
    0.4786286704993665,
    0.2369268850561891,
)


def lagrange_value(points, position, location):
    product_value = 1.0
    for other in range(len(points)):
        if other != position:
            product_value *= (location - points[other]) / (points[position] - points[other])
    return product_value


def lagrange_slope(points, position, location):
    slope_sum = 0.0
    for skipped in range(len(points)):
        if skipped == position:
            continue
        addend = 1.0 / (points[position] - points[skipped])
        for other in range(len(points)):
            if other != position and other != skipped:
                addend *= (location - points[other]) / (points[position] - points[other])
        slope_sum += addend
    return slope_sum


def along_axis(matrix, axis_id):
    eye = np.eye(NODES)
    parts = [eye, eye, eye]
    parts[axis_id] = matrix
    return np.kron(parts[0], np.kron(parts[1], parts[2]))


def tables():
    points = [0.5 * (value + 1.0) for value in GAUSS_POINTS]
    weights = np.array([0.5 * value for value in GAUSS_WEIGHTS])
    slopes = np.array([[lagrange_slope(points, p, points[q]) for p in range(NODES)] for q in range(NODES)])
    ends = [
        (
            np.array([lagrange_value(points, p, 0.0) for p in range(NODES)]),
            np.array([-lagrange_slope(points, p, 0.0) for p in range(NODES)]),
        ),
        (
            np.array([lagrange_value(points, p, 1.0) for p in range(NODES)]),
            np.array([lagrange_slope(points, p, 1.0) for p in range(NODES)]),
        ),
    ]
    cell_weight = np.kron(weights, np.kron(weights, weights))
    volume = sum(
        along_axis(slopes, a).T @ (cell_weight[:, None] * along_axis(slopes, a)) for a in range(3)
    )
    root = np.sqrt(0.5)
    modes = np.array(
        [
            [root, 0, 0, 0, root],
            [0, root, 0, root, 0],
            [0, 0, 1, 0, 0],
            [root, 0, 0, 0, -root],
            [0, root, 0, -root, 0],
        ]
    )
    modes = np.kron(modes, modes)
    mode_weight = np.array([weights[0], weights[1], weights[2], weights[0], weights[1]])
    mode_weight = np.kron(mode_weight, mode_weight)
    forward = np.zeros((6 * FACE + ROWS, ROWS))
    backward = np.zeros((ROWS, 6 * FACE))
    for face in range(6):
        trace, normal = ends[face % 2]
        trace = modes @ along_axis(trace[None, :], face // 2)
        normal = modes @ along_axis(normal[None, :], face // 2)
        row = face * FACE
        forward[row : row + 25, :BLOCK] = trace
        forward[row + 25, BLOCK] = 1.0
        forward[row + HALF : row + HALF + 25, :BLOCK] = normal
        backward[:BLOCK, row : row + 25] = trace.T * mode_weight
        backward[:BLOCK, row + HALF : row + HALF + 25] = -0.5 * normal.T * mode_weight
    forward[6 * FACE : 6 * FACE + BLOCK, :BLOCK] = volume
    face_rows = np.zeros(HALF)
    face_rows[:25] = mode_weight
    weight_rows = np.zeros((ROWS, 128))
    weight_rows[:BLOCK, 0] = cell_weight

    def halves(table):
        high = table.astype(ml_dtypes.bfloat16)
        return high, (table - high.astype(np.float64)).astype(ml_dtypes.bfloat16)

    weight_rows[: 2 * FACE, 1] = np.tile(np.concatenate([face_rows, -0.5 * face_rows]), 2)
    fwd_high, fwd_low = halves(forward)
    back_high, back_low = halves(backward)
    again = np.concatenate(halves(forward[: 2 * FACE] @ backward[:, : 2 * FACE]) + (np.zeros((ROWS, ROWS), ml_dtypes.bfloat16),), 1)
    return (
        np.concatenate([np.concatenate([fwd_high, fwd_high, fwd_low], 1), back_high, back_low, again], 0),
        weight_rows.astype(np.float32),
    )


def dot_nn(left, right):
    return jnp.dot(left, right, preferred_element_type=F32)


def dot_nt(left, right):
    return lax.dot_general(left, right, (((1,), (1,)), ((), ())), preferred_element_type=F32)


def split2(value):
    high = value.astype(BF16)
    return high, (value - high.astype(F32)).astype(BF16)


def split3(value):
    high = value.astype(BF16)
    rest = value - high.astype(F32)
    mid = rest.astype(BF16)
    return high, mid, (rest - mid.astype(F32)).astype(BF16)


def far_first(sizes):
    offsets = [tuple(int(i) for i in index) for index in np.ndindex(*sizes) if any(index)]
    offsets.sort(key=lambda index: -sum(min(i, n - i) for i, n in zip(index, sizes)))
    return [index[0] if len(sizes) == 1 else index for index in offsets]


def onehot(index_row, rows, start=0):
    ids = lax.broadcasted_iota(jnp.int32, (rows, index_row.shape[1]), 0) + start
    return jnp.where(ids == index_row, 1.0, 0.0).astype(BF16)


def kernel(
    n_curve, n_group, x_size,
    rs_hbm, cond_hbm, dest_hbm, nb_hbm, ori_hbm, sl_hbm, table_hbm, w_hbm,
    solution_out, residual_out,
    rs_ref, cond_ref, dest_ref, nb_ref, ori_ref, sl_ref, table_ref, w_ref, load_sem,
    b_ref, y_ref, z_ref, fb_ref, tail_ref, x3_ref, q_ref, g_ref, gg_ref, s_ref, sign_ref, f_ref, fs_ref, ch_ref, cl_ref,
    mig_send, mig_recv, halo_send, halo_recv, row_send, curve_recv, group_recv,
    mig_ssem, mig_rsem, halo_ssem, halo_rsem, curve_ssem, curve_rsem, group_ssem, group_rsem, one_sem, two_sem, plane_sem,
):
    curve = lax.axis_index("curve")
    group = lax.axis_index("group")
    me = curve * n_group + group
    total = n_curve * n_group
    has_left, has_right = me > 0, me < total - 1

    def device(rank):
        return (rank // n_group, lax.rem(rank, n_group))

    left, right = device(lax.rem(me + total - 1, total)), device(lax.rem(me + 1, total))
    z_size = n_group // x_size
    x_pos = lax.rem(group, x_size)
    z_pos = group // x_size
    curve_peers = [(lax.rem(curve + d, n_curve), group) for d in far_first((n_curve,))]
    group_peers = [
        (curve, lax.rem(z_pos + dz, z_size) * x_size + lax.rem(x_pos + dx, x_size))
        for dz, dx in far_first((z_size, x_size))
    ]
    y_size = n_curve // 2
    core = lax.rem(curve, 2)
    core_peer = (curve + 1 - 2 * core, group)

    def along(dim, offset):
        if dim == 0:
            return (curve, z_pos * x_size + lax.rem(x_pos + offset, x_size))
        if dim == 1:
            return (lax.rem(curve + 2 * offset, n_curve), group)
        return (curve, lax.rem(z_pos + offset, z_size) * x_size + x_pos)

    sizes = (x_size, y_size, z_size)
    near_peers = [core_peer] + [
        along(dim, offset) for dim in range(3) for offset in sorted({1, sizes[dim] - 1}) if sizes[dim] > 1
    ]

    def signal(sem, peer):
        pl.semaphore_signal(sem, inc=1, device_id=peer, device_id_type=MESH)

    def spread(reach, ring_sem):
        for dim in range(3):
            if sizes[dim] > 2 * reach + 1:
                signal(ring_sem.at[dim], along(dim, reach))
                signal(ring_sem.at[dim], along(dim, sizes[dim] - reach))

    def gather_known(reach, ring_sem):
        for dim in range(3):
            if sizes[dim] > 2 * reach + 1:
                pl.semaphore_wait(ring_sem.at[dim], 2)

    def two_away():
        gather_known(1, one_sem)
        spread(2, two_sem)

    def whole_plane():
        gather_known(2, two_sem)
        signal(plane_sem.at[0], core_peer)
        for offset in range(1, x_size):
            signal(plane_sem.at[1], along(0, offset))

    def before_sums():
        pl.semaphore_wait(plane_sem.at[0], 1)
        if x_size > 1:
            pl.semaphore_wait(plane_sem.at[1], x_size - 1)

    barrier = pltpu.get_barrier_semaphore()

    @pl.when(has_left)
    def _():
        signal(barrier, left)

    @pl.when(has_right)
    def _():
        signal(barrier, right)

    loads = {}
    for i, (name, source, sink) in enumerate(
        (
            ("dest", dest_hbm, dest_ref),
            ("rs", rs_hbm, rs_ref),
            ("cond", cond_hbm, cond_ref),
            ("nb", nb_hbm, nb_ref),
            ("sl", sl_hbm, sl_ref),
            ("ori", ori_hbm, ori_ref),
            ("table", table_hbm, table_ref),
            ("w", w_hbm, w_ref),
        )
    ):
        loads[name] = pltpu.make_async_copy(source, sink, load_sem.at[i])
        loads[name].start()
    for peer in near_peers:
        signal(barrier, peer)

    for start in range(0, CELLS, 64):
        ids = lax.broadcasted_iota(jnp.int32, (64, CELLS), 0) + start
        lanes = lax.broadcasted_iota(jnp.int32, (64, CELLS), 1)
        q_ref[start : start + 64, :] = jnp.where(ids <= lanes, 1.0, 0.0).astype(BF16)

    @pl.when(jnp.logical_not(has_left))
    def _():
        mig_recv[0:MOVE, :] = jnp.zeros((MOVE, ROWS), F32)
        halo_recv[:, 0] = jnp.zeros((2, FACE, GHOST), F32)

    @pl.when(jnp.logical_not(has_right))
    def _():
        mig_recv[MOVE:, :] = jnp.zeros((MOVE, ROWS), F32)
        halo_recv[:, 1] = jnp.zeros((2, FACE, GHOST), F32)

    loads["dest"].wait()

    destination = dest_ref[...]
    target = lax.shift_right_arithmetic(destination, 9) - me
    slot = jnp.bitwise_and(destination, CELLS - 1)
    row8 = lax.broadcasted_iota(jnp.int32, (8, CELLS), 0)
    leaving = jnp.where(((row8 == 0) & (target == -1)) | ((row8 == 1) & (target == 1)), 1.0, 0.0)
    counts = dot_nn(leaving.astype(BF16), q_ref[...]).astype(jnp.int32)
    place = jnp.where(target == -1, counts[0:1] - 1, jnp.where(target == 1, counts[1:2] + (MOVE - 1), -1))
    loads["rs"].wait()
    loads["cond"].wait()
    tail_ref[0:13, :] = rs_ref[112:BLOCK, :]
    tail_ref[13:14, :] = cond_ref[...]
    tail_ref[14:15, :] = (slot + 1).astype(F32)
    tail_ref[15:16, :] = jnp.zeros((1, CELLS), F32)
    for start, stop, value in ((0, 112, rs_ref[0:112, :]), (112, ROWS, tail_ref[...])):
        for i, part in enumerate(split3(value)):
            x3_ref[i * ROWS + start : i * ROWS + stop, :] = part
    packed = dot_nt(onehot(place, 2 * MOVE), x3_ref[...])
    mig_send[...] = packed[:, 0:ROWS] + packed[:, ROWS : 2 * ROWS] + packed[:, 2 * ROWS :]

    pl.semaphore_wait(barrier, len(near_peers) + has_left.astype(jnp.int32) + has_right.astype(jnp.int32))

    def copy(source, sink, ssem, rsem, peer):
        return pltpu.make_async_remote_copy(
            src_ref=source, dst_ref=sink, send_sem=ssem, recv_sem=rsem, device_id=peer, device_id_type=MESH
        )

    def start_both(to_left, to_right):
        pl.when(has_left)(to_left.start)
        pl.when(has_right)(to_right.start)

    to_left = copy(
        mig_send.at[pl.ds(0, MOVE)], mig_recv.at[pl.ds(MOVE, MOVE)], mig_ssem.at[0], mig_rsem.at[0], left
    )
    to_right = copy(
        mig_send.at[pl.ds(MOVE, MOVE)], mig_recv.at[pl.ds(0, MOVE)], mig_ssem.at[1], mig_rsem.at[1], right
    )
    start_both(to_left, to_right)
    spread(1, one_sem)
    loads["nb"].wait()
    loads["sl"].wait()
    loads["ori"].wait()

    def project(field, rows=slice(0, 2 * FACE)):
        high, low = field
        return dot_nn(table_ref[rows, 0:256], jnp.concatenate([high, low], 0)) + dot_nn(
            table_ref[rows, 256:384], high
        )

    def stack(face):
        high, low = split2(f_ref[face * FACE : (face + 1) * FACE, :])
        fs_ref[face, 0:FACE, :] = high
        fs_ref[face, FACE : 2 * FACE, :] = low

    def pair(product):
        return product[0:FACE] + product[FACE : 2 * FACE]

    def halo(step):
        return [
            copy(
                halo_send.at[step, side], halo_recv.at[step, 1 - side],
                halo_ssem.at[step, side], halo_rsem.at[step, side], peer,
            )
            for side, peer in ((0, left), (1, right))
        ]

    staying = jnp.where(target == 0, slot, -1)
    for start in range(0, CELLS, 64):
        q_ref[start : start + 64, :] = onehot(staying, 64, start)
    stay = dot_nt(x3_ref[...], q_ref[...])
    y_ref[...] = stay[0:ROWS] + stay[ROWS : 2 * ROWS] + stay[2 * ROWS :]
    for side in range(2):
        for start in range(0, CELLS, 128):
            s_ref[side, start : start + 128, :] = onehot(sl_ref[side : side + 1, :], 128, start)
    loads["table"].wait()
    loads["w"].wait()
    f_ref[0 : 2 * FACE, :] = project(split2(y_ref[...]))
    for side in range(2):
        stack(side)
        halo_send[0, side] = pair(dot_nn(fs_ref[side], s_ref[side]))
    mode = lax.broadcasted_iota(jnp.int32, (HALF, CELLS), 0)
    odd_first = jnp.where((mode >= 15) & (mode < 25), 2.0, 0.0)
    second = functools.reduce(jnp.logical_or, [mode == 5 * i + j for i in range(5) for j in (3, 4)])
    odd_second = jnp.where(second, 2.0, 0.0)
    outside = []
    for face in range(6):
        partner = nb_ref[face : face + 1, :]
        outside.append(jnp.where(partner < 0, 2.0, 1.0))
        for start in range(0, CELLS, 64):
            g_ref[face, start : start + 64, :] = onehot(partner, 64, start)
        if face < 2:
            for start in range(0, GHOST, 64):
                gg_ref[face, start : start + 64, :] = onehot(partner, 64, CELLS + face * GHOST + start)
        code = ori_ref[face : face + 1, :]
        first_bit = jnp.bitwise_and(code, 1).astype(F32)
        second_bit = lax.shift_right_arithmetic(code, 1).astype(F32)
        sign_ref[face] = (1.0 - odd_first * first_bit) * (1.0 - odd_second * second_bit)

    two_away()
    pl.when(has_left)(to_right.wait_recv)
    pl.when(has_right)(to_left.wait_recv)

    arrived = mig_recv[...].T
    slot_in = mig_recv[:, BLOCK + 1 : BLOCK + 2].astype(jnp.int32) - 1
    faces = project(split2(arrived))
    for side in range(2):
        listed = jnp.where(slot_in == sl_ref[side : side + 1, :], 1.0, 0.0).astype(BF16)
        parts = jnp.concatenate(split2(faces[side * FACE : (side + 1) * FACE]), 0)
        halo_send[0, side] += pair(dot_nn(parts, listed))
    copies_one = halo(0)
    start_both(*copies_one)

    place_in = arrived[BLOCK + 1 : BLOCK + 2, :].astype(jnp.int32) - 1
    for start in range(0, CELLS, 128):
        q_ref[start : start + 128, 0 : 2 * MOVE] = onehot(place_in, 128, start)
    moved = dot_nt(jnp.concatenate(split3(arrived), 0), q_ref[:, 0 : 2 * MOVE])
    field = y_ref[...] + (moved[0:ROWS] + moved[ROWS : 2 * ROWS] + moved[2 * ROWS :])
    conduct = field[BLOCK : BLOCK + 1, :]
    row_ids = lax.broadcasted_iota(jnp.int32, (ROWS, CELLS), 0)
    b_ref[...] = jnp.where(row_ids < BLOCK, field, 0.0)

    def with_conduct(value):
        return jnp.where(row_ids == BLOCK, conduct, value)

    def coefficients(face, near):
        row = face * FACE
        trace = f_ref[row : row + HALF, :]
        normal = f_ref[row + HALF : row + FACE, :]
        near_conduct = near[25:26, :]
        sign = sign_ref[face]
        near_value = sign * near[0:HALF]
        near_normal = sign * near[HALF:FACE]
        penalty = PENALTY * jnp.maximum(conduct, near_conduct)
        jump = outside[face] * trace - near_value
        first = (
            penalty * jump - (0.5 * outside[face] * conduct) * normal + (0.5 * near_conduct) * near_normal
        )
        parts = (first, conduct * jump)
        for offset, part in zip((0, HALF), parts):
            high, low = split2(part)
            ch_ref[row + offset : row + offset + HALF, :] = high
            cl_ref[row + offset : row + offset + HALF, :] = low
        return parts

    def expand(high, low, columns):
        return (
            dot_nn(high, ch_ref[columns, :])
            + dot_nn(high, cl_ref[columns, :])
            + dot_nn(low, ch_ref[columns, :])
        )

    def backward(start, stop):
        columns = slice(start * FACE, stop * FACE)
        return expand(table_ref[512:640, columns], table_ref[640:768, columns], columns)

    def local_part(value_ref, result_ref):
        for face in range(2, 6):
            stack(face)
        for face in range(2, 6):
            coefficients(face, pair(dot_nn(fs_ref[face ^ 1], g_ref[face])))
        local = [pair(dot_nn(fs_ref[face ^ 1], g_ref[face])) for face in range(2)]
        result_ref[...] = (
            w_ref[:, 0:1] * value_ref[...] + conduct * f_ref[6 * FACE :, :] + backward(2, 6)
        )
        return local

    def ghost_part(step, local, copies):
        parts = []
        for face in range(2):
            pl.when((has_left, has_right)[face])(copies[1 - face].wait_recv)
            high, low = split2(halo_recv[step, face])
            ghost = pair(dot_nn(jnp.concatenate([high, low], 0), gg_ref[face]))
            parts += coefficients(face, local[face] + ghost)
        return parts

    f_ref[...] = project(split2(with_conduct(b_ref[...])), slice(0, 6 * FACE + ROWS))
    fb_ref[...] = f_ref[0 : 2 * FACE, :]
    for side in range(2):
        stack(side)
    local = local_part(b_ref, y_ref)
    faces_ahead = project(split2(with_conduct(y_ref[...])))
    z_ref[...] = faces_ahead
    whole_plane()
    ghost_part(0, local, copies_one)
    f_ref[0 : 2 * FACE, :] = z_ref[...] + expand(
        table_ref[768:896, 0:128], table_ref[768:896, 128:256], slice(0, 2 * FACE)
    )
    for side in range(2):
        stack(side)
        halo_send[1, side] = pair(dot_nn(fs_ref[side], s_ref[side]))
    copies_two = halo(1)
    start_both(*copies_two)

    y_ref[...] += backward(0, 2)
    rest = slice(2 * FACE, 6 * FACE + ROWS)
    f_ref[rest, :] = project(split2(with_conduct(y_ref[...])), rest)
    local = local_part(y_ref, z_ref)

    def summed(terms):
        return jnp.sum(terms, axis=0, keepdims=True)

    source, image, partial = b_ref[...], y_ref[...], z_ref[...]
    early = [summed(source * source), summed(source * image), summed(image * image)]
    late = [summed(source * partial), summed(image * partial)]
    parts = jnp.concatenate(ghost_part(1, local, copies_two), 0) * w_ref[:, 1:2]
    late = [late[0] + summed(fb_ref[...] * parts), late[1] + summed(f_ref[0 : 2 * FACE, :] * parts)]
    lane = lax.broadcasted_iota(jnp.int32, (1, 128), 1)
    row = jnp.zeros((1, 128), F32)
    for index, terms in enumerate(early + late):
        row = row + jnp.where(lane == index, jnp.sum(terms, axis=1, keepdims=True), 0.0)

    before_sums()
    sent = []
    for phase, (peers, landing, ssem, rsem) in enumerate(
        (
            (curve_peers, curve_recv, curve_ssem, curve_rsem),
            (group_peers, group_recv, group_ssem, group_rsem),
        )
    ):
        row_send[phase] = row
        for i, peer in enumerate(peers):
            copy(row_send.at[phase], landing.at[i], ssem, rsem, peer).start()
        if phase == 0:
            z_ref[...] += backward(0, 2)
        every = copy(landing, landing, ssem, rsem, peers[0])
        every.wait_recv()
        terms = [row] + [landing[i] for i in range(len(peers))]
        while len(terms) > 1:
            terms = [sum(terms[i + 1 : i + 2], terms[i]) for i in range(0, len(terms), 2)]
        row = terms[0]
        sent.append(every)

    bb, by, yy, bz, yz = (
        jnp.sum(jnp.where(lane == index, row, 0.0), axis=1, keepdims=True) for index in range(5)
    )
    alpha = bb / by
    norm_next = bb - alpha * (2.0 * by - alpha * yy)
    beta = norm_next / bb
    grow = 1.0 + beta
    curvature = grow * (grow * by - alpha * (bz + yy)) + alpha * (alpha * yz)
    alpha_next = norm_next / curvature
    first = alpha + alpha_next * grow
    second = alpha * alpha_next
    source, image, second_image = b_ref[...], y_ref[...], z_ref[...]
    solution_out[...] = (first * source - second * image)[0:BLOCK]
    residual_out[...] = (source - first * image + second * second_image)[0:BLOCK]
    for one in sent:
        one.wait_send()
    for one_left, one_right in ((to_left, to_right), copies_one, copies_two):
        pl.when(has_left)(one_left.wait_send)
        pl.when(has_right)(one_right.wait_send)


def write_kernel(solution_ref, residual_ref, solution_out, residual_out, sem):
    copies = [
        pltpu.make_async_copy(solution_ref, solution_out, sem.at[0]),
        pltpu.make_async_copy(residual_ref, residual_out, sem.at[1]),
    ]
    for one in copies:
        one.start()
    for one in copies:
        one.wait()


def solution(mesh):
    n_curve, n_group = mesh.shape["curve"], mesh.shape["group"]
    x_size = min(X_SIZE, n_group)
    constants = tables()
    call = pl.pallas_call(
        functools.partial(kernel, n_curve, n_group, x_size),
        out_shape=(pltpu.VMEM((BLOCK, CELLS), F32), pltpu.VMEM((BLOCK, CELLS), F32)),
        in_specs=[pl.BlockSpec(memory_space=pl.ANY)] * 8,
        out_specs=[pl.BlockSpec(memory_space=pltpu.VMEM)] * 2,
        scratch_shapes=[
            pltpu.VMEM((BLOCK, CELLS), F32),
            pltpu.VMEM((1, CELLS), F32),
            pltpu.VMEM((1, CELLS), jnp.int32),
            pltpu.VMEM((6, CELLS), jnp.int32),
            pltpu.VMEM((6, CELLS), jnp.int32),
            pltpu.VMEM((2, GHOST), jnp.int32),
            *[pltpu.VMEM(table.shape, table.dtype) for table in constants],
            pltpu.SemaphoreType.DMA((8,)),
            pltpu.VMEM((ROWS, CELLS), F32),
            pltpu.VMEM((ROWS, CELLS), F32),
            pltpu.VMEM((ROWS, CELLS), F32),
            pltpu.VMEM((ROWS, CELLS), F32),
            pltpu.VMEM((16, CELLS), F32),
            pltpu.VMEM((3 * ROWS, CELLS), BF16),
            pltpu.VMEM((CELLS, CELLS), BF16),
            pltpu.VMEM((6, CELLS, CELLS), BF16),
            pltpu.VMEM((2, GHOST, CELLS), BF16),
            pltpu.VMEM((2, CELLS, GHOST), BF16),
            pltpu.VMEM((6, HALF, CELLS), F32),
            pltpu.VMEM((6 * FACE + ROWS, CELLS), F32),
            pltpu.VMEM((6, 2 * FACE, CELLS), BF16),
            pltpu.VMEM((6 * FACE, CELLS), BF16),
            pltpu.VMEM((6 * FACE, CELLS), BF16),
            pltpu.VMEM((2 * MOVE, ROWS), F32),
            pltpu.VMEM((2 * MOVE, ROWS), F32),
            pltpu.VMEM((2, 2, FACE, GHOST), F32),
            pltpu.VMEM((2, 2, FACE, GHOST), F32),
            pltpu.VMEM((2, 1, 128), F32),
            pltpu.VMEM((n_curve - 1, 1, 128), F32),
            pltpu.VMEM((n_group - 1, 1, 128), F32),
            pltpu.SemaphoreType.DMA((2,)),
            pltpu.SemaphoreType.DMA((2,)),
            pltpu.SemaphoreType.DMA((2, 2)),
            pltpu.SemaphoreType.DMA((2, 2)),
            pltpu.SemaphoreType.DMA,
            pltpu.SemaphoreType.DMA,
            pltpu.SemaphoreType.DMA,
            pltpu.SemaphoreType.DMA,
            pltpu.SemaphoreType.REGULAR((3,)),
            pltpu.SemaphoreType.REGULAR((3,)),
            pltpu.SemaphoreType.REGULAR((2,)),
        ],
        compiler_params=pltpu.CompilerParams(collective_id=0, has_side_effects=True),
    )

    field = jax.ShapeDtypeStruct((BLOCK, CELLS), F32)
    write = pl.pallas_call(
        write_kernel,
        out_shape=(field, field),
        in_specs=[pl.BlockSpec(memory_space=pltpu.VMEM)] * 2,
        out_specs=[pl.BlockSpec(memory_space=pl.ANY)] * 2,
        scratch_shapes=[pltpu.SemaphoreType.DMA((2,))],
    )

    def body(right_side, conductivity, destination, neighbour, orientation, send_list):
        fields = call(
            right_side, conductivity[None], destination[None], neighbour, orientation, send_list,
            *[jnp.asarray(table) for table in constants],
        )
        return write(*[pltpu.with_memory_space_constraint(one, pltpu.VMEM) for one in fields])

    in_specs = (
        P(None, CURVE_GROUP),
        P(CURVE_GROUP),
        P(CURVE_GROUP),
        P(None, CURVE_GROUP),
        P(None, CURVE_GROUP),
        P(None, CURVE_GROUP),
    )
    out_specs = (P(None, CURVE_GROUP), P(None, CURVE_GROUP))
    return jax.shard_map(body, mesh=mesh, in_specs=in_specs, out_specs=out_specs, check_vma=False)
```

```python
import functools

import jax
import jax.numpy as jnp
import ml_dtypes
import numpy as np
from jax import lax
from jax.experimental import pallas as pl
from jax.experimental.pallas import tpu as pltpu
from jax.sharding import PartitionSpec as P

NODES = 5
BLOCK = 125
CELLS = 512
GHOST = 256
MOVE = 64
PENALTY = 80.0
FACE = 64
HALF = 32
LISTED = HALF + 25
ROWS = 128
X_SIZE = 8
MESH = pl.DeviceIdType.MESH
F32 = jnp.float32
BF16 = jnp.bfloat16
CURVE_GROUP = ("curve", "group")
GAUSS_POINTS = (-0.906179845938664, -0.5384693101056831, 0.0, 0.5384693101056831, 0.906179845938664)
GAUSS_WEIGHTS = (
    0.2369268850561891,
    0.4786286704993665,
    0.5688888888888889,
    0.4786286704993665,
    0.2369268850561891,
)


def lagrange_value(points, position, location):
    product_value = 1.0
    for other in range(len(points)):
        if other != position:
            product_value *= (location - points[other]) / (points[position] - points[other])
    return product_value


def lagrange_slope(points, position, location):
    slope_sum = 0.0
    for skipped in range(len(points)):
        if skipped == position:
            continue
        addend = 1.0 / (points[position] - points[skipped])
        for other in range(len(points)):
            if other != position and other != skipped:
                addend *= (location - points[other]) / (points[position] - points[other])
        slope_sum += addend
    return slope_sum


def along_axis(matrix, axis_id):
    eye = np.eye(NODES)
    parts = [eye, eye, eye]
    parts[axis_id] = matrix
    return np.kron(parts[0], np.kron(parts[1], parts[2]))


def tables():
    points = [0.5 * (value + 1.0) for value in GAUSS_POINTS]
    weights = np.array([0.5 * value for value in GAUSS_WEIGHTS])
    slopes = np.array([[lagrange_slope(points, p, points[q]) for p in range(NODES)] for q in range(NODES)])
    ends = [
        (
            np.array([lagrange_value(points, p, 0.0) for p in range(NODES)]),
            np.array([-lagrange_slope(points, p, 0.0) for p in range(NODES)]),
        ),
        (
            np.array([lagrange_value(points, p, 1.0) for p in range(NODES)]),
            np.array([lagrange_slope(points, p, 1.0) for p in range(NODES)]),
        ),
    ]
    cell_weight = np.kron(weights, np.kron(weights, weights))
    volume = sum(
        along_axis(slopes, a).T @ (cell_weight[:, None] * along_axis(slopes, a)) for a in range(3)
    )
    root = np.sqrt(0.5)
    modes = np.array(
        [
            [root, 0, 0, 0, root],
            [0, root, 0, root, 0],
            [0, 0, 1, 0, 0],
            [root, 0, 0, 0, -root],
            [0, root, 0, -root, 0],
        ]
    )
    modes = np.kron(modes, modes)
    mode_weight = np.array([weights[0], weights[1], weights[2], weights[0], weights[1]])
    mode_weight = np.kron(mode_weight, mode_weight)
    forward = np.zeros((6 * FACE + ROWS, ROWS))
    backward = np.zeros((ROWS, 6 * FACE))
    for face in range(6):
        trace, normal = ends[face % 2]
        trace = modes @ along_axis(trace[None, :], face // 2)
        normal = modes @ along_axis(normal[None, :], face // 2)
        row = face * FACE
        forward[row : row + 25, :BLOCK] = trace
        forward[row + 25, BLOCK] = 1.0
        forward[row + HALF : row + HALF + 25, :BLOCK] = normal
        backward[:BLOCK, row : row + 25] = trace.T * mode_weight
        backward[:BLOCK, row + HALF : row + HALF + 25] = -0.5 * normal.T * mode_weight
    forward[6 * FACE : 6 * FACE + BLOCK, :BLOCK] = volume
    face_rows = np.zeros(HALF)
    face_rows[:25] = mode_weight
    weight_rows = np.zeros((ROWS, 128))
    weight_rows[:BLOCK, 0] = cell_weight

    def halves(table):
        high = table.astype(ml_dtypes.bfloat16)
        return high, (table - high.astype(np.float64)).astype(ml_dtypes.bfloat16)

    weight_rows[: 2 * FACE, 1] = np.tile(np.concatenate([face_rows, -0.5 * face_rows]), 2)
    fwd_high, fwd_low = halves(forward)
    back_high, back_low = halves(backward)
    again = np.concatenate(halves(forward[: 2 * FACE] @ backward[:, : 2 * FACE]) + (np.zeros((ROWS, ROWS), ml_dtypes.bfloat16),), 1)
    return (
        np.concatenate([np.concatenate([fwd_high, fwd_high, fwd_low], 1), back_high, back_low, again], 0),
        weight_rows.astype(np.float32),
    )


def dot_nn(left, right):
    return jnp.dot(left, right, preferred_element_type=F32)


def dot_nt(left, right):
    return lax.dot_general(left, right, (((1,), (1,)), ((), ())), preferred_element_type=F32)


def split2(value):
    high = value.astype(BF16)
    return high, (value - high.astype(F32)).astype(BF16)


def split3(value):
    high = value.astype(BF16)
    rest = value - high.astype(F32)
    mid = rest.astype(BF16)
    return high, mid, (rest - mid.astype(F32)).astype(BF16)


def far_first(sizes):
    offsets = [tuple(int(i) for i in index) for index in np.ndindex(*sizes) if any(index)]
    offsets.sort(key=lambda index: -sum(min(i, n - i) for i, n in zip(index, sizes)))
    return [index[0] if len(sizes) == 1 else index for index in offsets]


def onehot(index_row, rows, start=0):
    ids = lax.broadcasted_iota(jnp.int32, (rows, index_row.shape[1]), 0) + start
    return jnp.where(ids == index_row, 1.0, 0.0).astype(BF16)


def kernel(
    n_curve, n_group, x_size,
    rs_hbm, cond_hbm, dest_hbm, nb_hbm, ori_hbm, sl_hbm, table_hbm, w_hbm,
    solution_out, residual_out,
    rs_ref, cond_ref, dest_ref, nb_ref, ori_ref, sl_ref, table_ref, w_ref, load_sem,
    b_ref, y_ref, z_ref, fb_ref, tail_ref, x3_ref, q_ref, g_ref, gg_ref, s_ref, sign_ref, f_ref, fs_ref, ch_ref, cl_ref,
    mig_send, mig_recv, far_recv, halo_send, halo_recv, row_send, curve_recv, group_recv,
    mig_ssem, mig_rsem, far_ssem, far_rsem, halo_ssem, halo_rsem, curve_ssem, curve_rsem, group_ssem, group_rsem, one_sem, two_sem, plane_sem,
):
    curve = lax.axis_index("curve")
    group = lax.axis_index("group")
    me = curve * n_group + group
    total = n_curve * n_group
    has_left, has_right = me > 0, me < total - 1
    edge_left, edge_right = (group == 0) & has_left, (group == n_group - 1) & has_right
    plain_left = has_left & jnp.logical_not(edge_left)
    plain_right = has_right & jnp.logical_not(edge_right)
    far_left = (group == 1) & (curve > 0)
    far_right = (group == n_group - 2) & (curve < n_curve - 1)

    def device(rank):
        return (rank // n_group, lax.rem(rank, n_group))

    left, right = device(lax.rem(me + total - 1, total)), device(lax.rem(me + 1, total))
    left_two, right_two = device(lax.rem(me + total - 2, total)), device(lax.rem(me + 2, total))
    z_size = n_group // x_size
    x_pos = lax.rem(group, x_size)
    z_pos = group // x_size
    curve_peers = [(lax.rem(curve + d, n_curve), group) for d in far_first((n_curve,))]
    group_peers = [
        (curve, lax.rem(z_pos + dz, z_size) * x_size + lax.rem(x_pos + dx, x_size))
        for dz, dx in far_first((z_size, x_size))
    ]
    y_size = n_curve // 2
    core = lax.rem(curve, 2)
    core_peer = (curve + 1 - 2 * core, group)

    def along(dim, offset):
        if dim == 0:
            return (curve, z_pos * x_size + lax.rem(x_pos + offset, x_size))
        if dim == 1:
            return (lax.rem(curve + 2 * offset, n_curve), group)
        return (curve, lax.rem(z_pos + offset, z_size) * x_size + x_pos)

    sizes = (x_size, y_size, z_size)
    near_peers = [core_peer] + [
        along(dim, offset) for dim in range(3) for offset in sorted({1, sizes[dim] - 1}) if sizes[dim] > 1
    ]

    def signal(sem, peer):
        pl.semaphore_signal(sem, inc=1, device_id=peer, device_id_type=MESH)

    def spread(reach, ring_sem):
        for dim in range(3):
            if sizes[dim] > 2 * reach + 1:
                signal(ring_sem.at[dim], along(dim, reach))
                signal(ring_sem.at[dim], along(dim, sizes[dim] - reach))

    def gather_known(reach, ring_sem):
        for dim in range(3):
            if sizes[dim] > 2 * reach + 1:
                pl.semaphore_wait(ring_sem.at[dim], 2)

    def two_away():
        gather_known(1, one_sem)
        spread(2, two_sem)

    def whole_plane():
        gather_known(2, two_sem)
        signal(plane_sem.at[0], core_peer)
        for offset in range(1, x_size):
            signal(plane_sem.at[1], along(0, offset))

    def before_sums():
        pl.semaphore_wait(plane_sem.at[0], 1)
        if x_size > 1:
            pl.semaphore_wait(plane_sem.at[1], x_size - 1)

    barrier = pltpu.get_barrier_semaphore()

    @pl.when(has_left)
    def _():
        signal(barrier, left)

    @pl.when(has_right)
    def _():
        signal(barrier, right)

    @pl.when(edge_left)
    def _():
        signal(barrier, left_two)

    @pl.when(edge_right)
    def _():
        signal(barrier, right_two)

    loads = {}
    for i, (name, source, sink) in enumerate(
        (
            ("dest", dest_hbm, dest_ref),
            ("rs", rs_hbm, rs_ref),
            ("cond", cond_hbm, cond_ref),
            ("nb", nb_hbm, nb_ref),
            ("sl", sl_hbm, sl_ref),
            ("ori", ori_hbm, ori_ref),
            ("table", table_hbm, table_ref),
            ("w", w_hbm, w_ref),
        )
    ):
        loads[name] = pltpu.make_async_copy(source, sink, load_sem.at[i])
        loads[name].start()
    for peer in near_peers:
        signal(barrier, peer)

    for start in range(0, CELLS, 64):
        ids = lax.broadcasted_iota(jnp.int32, (64, CELLS), 0) + start
        lanes = lax.broadcasted_iota(jnp.int32, (64, CELLS), 1)
        q_ref[start : start + 64, :] = jnp.where(ids <= lanes, 1.0, 0.0).astype(BF16)

    @pl.when(jnp.logical_not(has_left))
    def _():
        mig_recv[0:MOVE, :] = jnp.zeros((MOVE, ROWS), F32)
        halo_recv[:, 0] = jnp.zeros((2, FACE, GHOST), F32)

    @pl.when(jnp.logical_not(has_right))
    def _():
        mig_recv[MOVE:, :] = jnp.zeros((MOVE, ROWS), F32)
        halo_recv[:, 1] = jnp.zeros((2, FACE, GHOST), F32)

    loads["dest"].wait()

    destination = dest_ref[...]
    target = lax.shift_right_arithmetic(destination, 9) - me
    slot = jnp.bitwise_and(destination, CELLS - 1)
    row8 = lax.broadcasted_iota(jnp.int32, (8, CELLS), 0)
    leaving = jnp.where(((row8 == 0) & (target == -1)) | ((row8 == 1) & (target == 1)), 1.0, 0.0)
    counts = dot_nn(leaving.astype(BF16), q_ref[...]).astype(jnp.int32)
    place = jnp.where(target == -1, counts[0:1] - 1, jnp.where(target == 1, counts[1:2] + (MOVE - 1), -1))
    loads["rs"].wait()
    loads["cond"].wait()
    tail_ref[0:13, :] = rs_ref[112:BLOCK, :]
    tail_ref[13:14, :] = cond_ref[...]
    tail_ref[14:15, :] = (slot + 1).astype(F32)
    tail_ref[15:16, :] = jnp.zeros((1, CELLS), F32)
    for start, stop, value in ((0, 112, rs_ref[0:112, :]), (112, ROWS, tail_ref[...])):
        for i, part in enumerate(split3(value)):
            x3_ref[i * ROWS + start : i * ROWS + stop, :] = part
    packed = dot_nt(onehot(place, 2 * MOVE), x3_ref[...])
    mig_send[...] = packed[:, 0:ROWS] + packed[:, ROWS : 2 * ROWS] + packed[:, 2 * ROWS :]

    greeted = [has_left, has_right, far_left, far_right]
    pl.semaphore_wait(barrier, len(near_peers) + sum(one.astype(jnp.int32) for one in greeted))

    def copy(source, sink, ssem, rsem, peer):
        return pltpu.make_async_remote_copy(
            src_ref=source, dst_ref=sink, send_sem=ssem, recv_sem=rsem, device_id=peer, device_id_type=MESH
        )

    def start_both(to_left, to_right):
        pl.when(has_left)(to_left.start)
        pl.when(has_right)(to_right.start)

    to_left = copy(
        mig_send.at[pl.ds(0, MOVE)], mig_recv.at[pl.ds(MOVE, MOVE)], mig_ssem.at[0], mig_rsem.at[0], left
    )
    to_right = copy(
        mig_send.at[pl.ds(MOVE, MOVE)], mig_recv.at[pl.ds(0, MOVE)], mig_ssem.at[1], mig_rsem.at[1], right
    )
    start_both(to_left, to_right)
    to_far_left = copy(mig_send.at[pl.ds(0, MOVE)], far_recv, far_ssem.at[0], far_rsem, left_two)
    to_far_right = copy(mig_send.at[pl.ds(MOVE, MOVE)], far_recv, far_ssem.at[1], far_rsem, right_two)
    pl.when(far_left)(to_far_left.start)
    pl.when(far_right)(to_far_right.start)
    spread(1, one_sem)
    loads["nb"].wait()
    loads["sl"].wait()
    loads["ori"].wait()

    def project(field, rows=slice(0, 2 * FACE)):
        high, low = field
        return dot_nn(table_ref[rows, 0:256], jnp.concatenate([high, low], 0)) + dot_nn(
            table_ref[rows, 256:384], high
        )

    def stack(face):
        high, low = split2(f_ref[face * FACE : (face + 1) * FACE, :])
        fs_ref[face, 0:FACE, :] = high
        fs_ref[face, FACE : 2 * FACE, :] = low

    def pair(product):
        return product[0:FACE] + product[FACE : 2 * FACE]

    def halo(step):
        return [
            copy(
                halo_send.at[step, side], halo_recv.at[step, 1 - side],
                halo_ssem.at[step, side], halo_rsem.at[step, side], peer,
            )
            for side, peer in ((0, left), (1, right))
        ]

    staying = jnp.where(target == 0, slot, -1)
    for start in range(0, CELLS, 64):
        q_ref[start : start + 64, :] = onehot(staying, 64, start)
    stay = dot_nt(x3_ref[...], q_ref[...])
    y_ref[...] = stay[0:ROWS] + stay[ROWS : 2 * ROWS] + stay[2 * ROWS :]
    for side in range(2):
        for start in range(0, CELLS, 128):
            s_ref[side, start : start + 128, :] = onehot(sl_ref[side : side + 1, :], 128, start)
    loads["table"].wait()
    loads["w"].wait()
    f_ref[0 : 2 * FACE, :] = project(split2(y_ref[...]))
    for side in range(2):
        stack(side)
        halo_send[0, side] = pair(dot_nn(fs_ref[side], s_ref[side]))
        halo_send[0, side, LISTED : LISTED + 1, :] = sl_ref[side : side + 1, :].astype(F32)
    copies_one = halo(0)
    pl.when(edge_left)(copies_one[0].start)
    pl.when(edge_right)(copies_one[1].start)
    mode = lax.broadcasted_iota(jnp.int32, (HALF, CELLS), 0)
    odd_first = jnp.where((mode >= 15) & (mode < 25), 2.0, 0.0)
    second = functools.reduce(jnp.logical_or, [mode == 5 * i + j for i in range(5) for j in (3, 4)])
    odd_second = jnp.where(second, 2.0, 0.0)
    outside = []
    for face in range(6):
        partner = nb_ref[face : face + 1, :]
        outside.append(jnp.where(partner < 0, 2.0, 1.0))
        for start in range(0, CELLS, 64):
            g_ref[face, start : start + 64, :] = onehot(partner, 64, start)
        if face < 2:
            for start in range(0, GHOST, 64):
                gg_ref[face, start : start + 64, :] = onehot(partner, 64, CELLS + face * GHOST + start)
        code = ori_ref[face : face + 1, :]
        first_bit = jnp.bitwise_and(code, 1).astype(F32)
        second_bit = lax.shift_right_arithmetic(code, 1).astype(F32)
        sign_ref[face] = (1.0 - odd_first * first_bit) * (1.0 - odd_second * second_bit)

    two_away()
    pl.when(has_left)(to_right.wait_recv)
    pl.when(has_right)(to_left.wait_recv)

    arrived = mig_recv[...].T
    faces = project(split2(arrived))

    def place_faces(faces, records, listed):
        slots = records[:, BLOCK + 1 : BLOCK + 2].astype(jnp.int32) - 1
        chosen = jnp.where(slots == listed, 1.0, 0.0).astype(BF16)
        return pair(dot_nn(jnp.concatenate(split2(faces), 0), chosen))

    came = mig_recv[...]
    for side, plain in ((0, plain_left), (1, plain_right)):
        more = place_faces(faces[side * FACE : (side + 1) * FACE], came, sl_ref[side : side + 1, :])

        @pl.when(plain)
        def _():
            halo_send[0, side] += more

    pl.when(plain_left)(copies_one[0].start)
    pl.when(plain_right)(copies_one[1].start)

    place_in = arrived[BLOCK + 1 : BLOCK + 2, :].astype(jnp.int32) - 1
    for start in range(0, CELLS, 128):
        q_ref[start : start + 128, 0 : 2 * MOVE] = onehot(place_in, 128, start)
    moved = dot_nt(jnp.concatenate(split3(arrived), 0), q_ref[:, 0 : 2 * MOVE])
    field = y_ref[...] + (moved[0:ROWS] + moved[ROWS : 2 * ROWS] + moved[2 * ROWS :])
    conduct = field[BLOCK : BLOCK + 1, :]
    row_ids = lax.broadcasted_iota(jnp.int32, (ROWS, CELLS), 0)
    b_ref[...] = jnp.where(row_ids < BLOCK, field, 0.0)

    def with_conduct(value):
        return jnp.where(row_ids == BLOCK, conduct, value)

    def coefficients(face, near):
        row = face * FACE
        trace = f_ref[row : row + HALF, :]
        normal = f_ref[row + HALF : row + FACE, :]
        near_conduct = near[25:26, :]
        sign = sign_ref[face]
        near_value = sign * near[0:HALF]
        near_normal = sign * near[HALF:FACE]
        penalty = PENALTY * jnp.maximum(conduct, near_conduct)
        jump = outside[face] * trace - near_value
        first = (
            penalty * jump - (0.5 * outside[face] * conduct) * normal + (0.5 * near_conduct) * near_normal
        )
        parts = (first, conduct * jump)
        for offset, part in zip((0, HALF), parts):
            high, low = split2(part)
            ch_ref[row + offset : row + offset + HALF, :] = high
            cl_ref[row + offset : row + offset + HALF, :] = low
        return parts

    def expand(high, low, columns):
        return (
            dot_nn(high, ch_ref[columns, :])
            + dot_nn(high, cl_ref[columns, :])
            + dot_nn(low, ch_ref[columns, :])
        )

    def backward(start, stop):
        columns = slice(start * FACE, stop * FACE)
        return expand(table_ref[512:640, columns], table_ref[640:768, columns], columns)

    def local_part(value_ref, result_ref):
        for face in range(2, 6):
            stack(face)
        for face in range(2, 6):
            coefficients(face, pair(dot_nn(fs_ref[face ^ 1], g_ref[face])))
        local = [pair(dot_nn(fs_ref[face ^ 1], g_ref[face])) for face in range(2)]
        result_ref[...] = (
            w_ref[:, 0:1] * value_ref[...] + conduct * f_ref[6 * FACE :, :] + backward(2, 6)
        )
        return local

    def complete(face, incoming):
        incoming.wait_recv()
        to_far_left.wait_recv()
        records = jnp.concatenate([mig_send[face * MOVE : (face + 1) * MOVE, :], far_recv[...]], 0)
        other = 1 - face
        faces = project(split2(records.T), slice(other * FACE, (other + 1) * FACE))
        listed = halo_recv[0, face, LISTED : LISTED + 1, :].astype(jnp.int32)
        halo_recv[0, face] += place_faces(faces, records, listed)

    def ghost_part(step, local, copies):
        parts = []
        for face in range(2):
            if step == 0:
                pl.when((plain_left, plain_right)[face])(copies[1 - face].wait_recv)
                pl.when((edge_left, edge_right)[face])(functools.partial(complete, face, copies[1 - face]))
            else:
                pl.when((has_left, has_right)[face])(copies[1 - face].wait_recv)
            high, low = split2(halo_recv[step, face])
            ghost = pair(dot_nn(jnp.concatenate([high, low], 0), gg_ref[face]))
            parts += coefficients(face, local[face] + ghost)
        return parts

    f_ref[...] = project(split2(with_conduct(b_ref[...])), slice(0, 6 * FACE + ROWS))
    fb_ref[...] = f_ref[0 : 2 * FACE, :]
    for side in range(2):
        stack(side)
    local = local_part(b_ref, y_ref)
    faces_ahead = project(split2(with_conduct(y_ref[...])))
    z_ref[...] = faces_ahead
    whole_plane()
    ghost_part(0, local, copies_one)
    f_ref[0 : 2 * FACE, :] = z_ref[...] + expand(
        table_ref[768:896, 0:128], table_ref[768:896, 128:256], slice(0, 2 * FACE)
    )
    for side in range(2):
        stack(side)
        halo_send[1, side] = pair(dot_nn(fs_ref[side], s_ref[side]))
    copies_two = halo(1)
    start_both(*copies_two)

    y_ref[...] += backward(0, 2)
    rest = slice(2 * FACE, 6 * FACE + ROWS)
    f_ref[rest, :] = project(split2(with_conduct(y_ref[...])), rest)
    local = local_part(y_ref, z_ref)

    def summed(terms):
        return jnp.sum(terms, axis=0, keepdims=True)

    source, image, partial = b_ref[...], y_ref[...], z_ref[...]
    early = [summed(source * source), summed(source * image), summed(image * image)]
    late = [summed(source * partial), summed(image * partial)]
    parts = jnp.concatenate(ghost_part(1, local, copies_two), 0) * w_ref[:, 1:2]
    late = [late[0] + summed(fb_ref[...] * parts), late[1] + summed(f_ref[0 : 2 * FACE, :] * parts)]
    lane = lax.broadcasted_iota(jnp.int32, (1, 128), 1)
    row = jnp.zeros((1, 128), F32)
    for index, terms in enumerate(early + late):
        row = row + jnp.where(lane == index, jnp.sum(terms, axis=1, keepdims=True), 0.0)

    before_sums()
    sent = []
    for phase, (peers, landing, ssem, rsem) in enumerate(
        (
            (curve_peers, curve_recv, curve_ssem, curve_rsem),
            (group_peers, group_recv, group_ssem, group_rsem),
        )
    ):
        row_send[phase] = row
        for i, peer in enumerate(peers):
            copy(row_send.at[phase], landing.at[i], ssem, rsem, peer).start()
        if phase == 0:
            z_ref[...] += backward(0, 2)
        every = copy(landing, landing, ssem, rsem, peers[0])
        every.wait_recv()
        terms = [row] + [landing[i] for i in range(len(peers))]
        while len(terms) > 1:
            terms = [sum(terms[i + 1 : i + 2], terms[i]) for i in range(0, len(terms), 2)]
        row = terms[0]
        sent.append(every)

    bb, by, yy, bz, yz = (
        jnp.sum(jnp.where(lane == index, row, 0.0), axis=1, keepdims=True) for index in range(5)
    )
    alpha = bb / by
    norm_next = bb - alpha * (2.0 * by - alpha * yy)
    beta = norm_next / bb
    grow = 1.0 + beta
    curvature = grow * (grow * by - alpha * (bz + yy)) + alpha * (alpha * yz)
    alpha_next = norm_next / curvature
    first = alpha + alpha_next * grow
    second = alpha * alpha_next
    source, image, second_image = b_ref[...], y_ref[...], z_ref[...]
    solution_out[...] = (first * source - second * image)[0:BLOCK]
    residual_out[...] = (source - first * image + second * second_image)[0:BLOCK]
    for one in sent:
        one.wait_send()
    pl.when(far_left)(to_far_left.wait_send)
    pl.when(far_right)(to_far_right.wait_send)
    for one_left, one_right in ((to_left, to_right), copies_one, copies_two):
        pl.when(has_left)(one_left.wait_send)
        pl.when(has_right)(one_right.wait_send)


def write_kernel(solution_ref, residual_ref, solution_out, residual_out, sem):
    copies = [
        pltpu.make_async_copy(solution_ref, solution_out, sem.at[0]),
        pltpu.make_async_copy(residual_ref, residual_out, sem.at[1]),
    ]
    for one in copies:
        one.start()
    for one in copies:
        one.wait()


def solution(mesh):
    n_curve, n_group = mesh.shape["curve"], mesh.shape["group"]
    x_size = min(X_SIZE, n_group)
    constants = tables()
    call = pl.pallas_call(
        functools.partial(kernel, n_curve, n_group, x_size),
        out_shape=(pltpu.VMEM((BLOCK, CELLS), F32), pltpu.VMEM((BLOCK, CELLS), F32)),
        in_specs=[pl.BlockSpec(memory_space=pl.ANY)] * 8,
        out_specs=[pl.BlockSpec(memory_space=pltpu.VMEM)] * 2,
        scratch_shapes=[
            pltpu.VMEM((BLOCK, CELLS), F32),
            pltpu.VMEM((1, CELLS), F32),
            pltpu.VMEM((1, CELLS), jnp.int32),
            pltpu.VMEM((6, CELLS), jnp.int32),
            pltpu.VMEM((6, CELLS), jnp.int32),
            pltpu.VMEM((2, GHOST), jnp.int32),
            *[pltpu.VMEM(table.shape, table.dtype) for table in constants],
            pltpu.SemaphoreType.DMA((8,)),
            pltpu.VMEM((ROWS, CELLS), F32),
            pltpu.VMEM((ROWS, CELLS), F32),
            pltpu.VMEM((ROWS, CELLS), F32),
            pltpu.VMEM((ROWS, CELLS), F32),
            pltpu.VMEM((16, CELLS), F32),
            pltpu.VMEM((3 * ROWS, CELLS), BF16),
            pltpu.VMEM((CELLS, CELLS), BF16),
            pltpu.VMEM((6, CELLS, CELLS), BF16),
            pltpu.VMEM((2, GHOST, CELLS), BF16),
            pltpu.VMEM((2, CELLS, GHOST), BF16),
            pltpu.VMEM((6, HALF, CELLS), F32),
            pltpu.VMEM((6 * FACE + ROWS, CELLS), F32),
            pltpu.VMEM((6, 2 * FACE, CELLS), BF16),
            pltpu.VMEM((6 * FACE, CELLS), BF16),
            pltpu.VMEM((6 * FACE, CELLS), BF16),
            pltpu.VMEM((2 * MOVE, ROWS), F32),
            pltpu.VMEM((2 * MOVE, ROWS), F32),
            pltpu.VMEM((MOVE, ROWS), F32),
            pltpu.VMEM((2, 2, FACE, GHOST), F32),
            pltpu.VMEM((2, 2, FACE, GHOST), F32),
            pltpu.VMEM((2, 1, 128), F32),
            pltpu.VMEM((n_curve - 1, 1, 128), F32),
            pltpu.VMEM((n_group - 1, 1, 128), F32),
            pltpu.SemaphoreType.DMA((2,)),
            pltpu.SemaphoreType.DMA((2,)),
            pltpu.SemaphoreType.DMA((2,)),
            pltpu.SemaphoreType.DMA,
            pltpu.SemaphoreType.DMA((2, 2)),
            pltpu.SemaphoreType.DMA((2, 2)),
            pltpu.SemaphoreType.DMA,
            pltpu.SemaphoreType.DMA,
            pltpu.SemaphoreType.DMA,
            pltpu.SemaphoreType.DMA,
            pltpu.SemaphoreType.REGULAR((3,)),
            pltpu.SemaphoreType.REGULAR((3,)),
            pltpu.SemaphoreType.REGULAR((2,)),
        ],
        compiler_params=pltpu.CompilerParams(collective_id=0, has_side_effects=True),
    )

    field = jax.ShapeDtypeStruct((BLOCK, CELLS), F32)
    write = pl.pallas_call(
        write_kernel,
        out_shape=(field, field),
        in_specs=[pl.BlockSpec(memory_space=pltpu.VMEM)] * 2,
        out_specs=[pl.BlockSpec(memory_space=pl.ANY)] * 2,
        scratch_shapes=[pltpu.SemaphoreType.DMA((2,))],
    )

    def body(right_side, conductivity, destination, neighbour, orientation, send_list):
        fields = call(
            right_side, conductivity[None], destination[None], neighbour, orientation, send_list,
            *[jnp.asarray(table) for table in constants],
        )
        return write(*[pltpu.with_memory_space_constraint(one, pltpu.VMEM) for one in fields])

    in_specs = (
        P(None, CURVE_GROUP),
        P(CURVE_GROUP),
        P(CURVE_GROUP),
        P(None, CURVE_GROUP),
        P(None, CURVE_GROUP),
        P(None, CURVE_GROUP),
    )
    out_specs = (P(None, CURVE_GROUP), P(None, CURVE_GROUP))
    return jax.shard_map(body, mesh=mesh, in_specs=in_specs, out_specs=out_specs, check_vma=False)
```

```python
import functools

import jax
import jax.numpy as jnp
import ml_dtypes
import numpy as np
from jax import lax
from jax.experimental import pallas as pl
from jax.experimental.pallas import tpu as pltpu
from jax.sharding import PartitionSpec as P

NODES = 5
BLOCK = 125
CELLS = 512
GHOST = 256
MOVE = 64
PENALTY = 80.0
FACE = 64
HALF = 32
LISTED = HALF + 25
ROWS = 128
X_SIZE = 8
MESH = pl.DeviceIdType.MESH
F32 = jnp.float32
BF16 = jnp.bfloat16
CURVE_GROUP = ("curve", "group")
GAUSS_POINTS = (-0.906179845938664, -0.5384693101056831, 0.0, 0.5384693101056831, 0.906179845938664)
GAUSS_WEIGHTS = (
    0.2369268850561891,
    0.4786286704993665,
    0.5688888888888889,
    0.4786286704993665,
    0.2369268850561891,
)


def lagrange_value(points, position, location):
    product_value = 1.0
    for other in range(len(points)):
        if other != position:
            product_value *= (location - points[other]) / (points[position] - points[other])
    return product_value


def lagrange_slope(points, position, location):
    slope_sum = 0.0
    for skipped in range(len(points)):
        if skipped == position:
            continue
        addend = 1.0 / (points[position] - points[skipped])
        for other in range(len(points)):
            if other != position and other != skipped:
                addend *= (location - points[other]) / (points[position] - points[other])
        slope_sum += addend
    return slope_sum


def along_axis(matrix, axis_id):
    eye = np.eye(NODES)
    parts = [eye, eye, eye]
    parts[axis_id] = matrix
    return np.kron(parts[0], np.kron(parts[1], parts[2]))


def tables():
    points = [0.5 * (value + 1.0) for value in GAUSS_POINTS]
    weights = np.array([0.5 * value for value in GAUSS_WEIGHTS])
    slopes = np.array([[lagrange_slope(points, p, points[q]) for p in range(NODES)] for q in range(NODES)])
    ends = [
        (
            np.array([lagrange_value(points, p, 0.0) for p in range(NODES)]),
            np.array([-lagrange_slope(points, p, 0.0) for p in range(NODES)]),
        ),
        (
            np.array([lagrange_value(points, p, 1.0) for p in range(NODES)]),
            np.array([lagrange_slope(points, p, 1.0) for p in range(NODES)]),
        ),
    ]
    cell_weight = np.kron(weights, np.kron(weights, weights))
    volume = sum(
        along_axis(slopes, a).T @ (cell_weight[:, None] * along_axis(slopes, a)) for a in range(3)
    )
    root = np.sqrt(0.5)
    modes = np.array(
        [
            [root, 0, 0, 0, root],
            [0, root, 0, root, 0],
            [0, 0, 1, 0, 0],
            [root, 0, 0, 0, -root],
            [0, root, 0, -root, 0],
        ]
    )
    modes = np.kron(modes, modes)
    mode_weight = np.array([weights[0], weights[1], weights[2], weights[0], weights[1]])
    mode_weight = np.kron(mode_weight, mode_weight)
    forward = np.zeros((6 * FACE + ROWS, ROWS))
    backward = np.zeros((ROWS, 6 * FACE))
    for face in range(6):
        trace, normal = ends[face % 2]
        trace = modes @ along_axis(trace[None, :], face // 2)
        normal = modes @ along_axis(normal[None, :], face // 2)
        row = face * FACE
        forward[row : row + 25, :BLOCK] = trace
        forward[row + 25, BLOCK] = 1.0
        forward[row + HALF : row + HALF + 25, :BLOCK] = normal
        backward[:BLOCK, row : row + 25] = trace.T * mode_weight
        backward[:BLOCK, row + HALF : row + HALF + 25] = -0.5 * normal.T * mode_weight
    forward[6 * FACE : 6 * FACE + BLOCK, :BLOCK] = volume
    face_rows = np.zeros(HALF)
    face_rows[:25] = mode_weight
    weight_rows = np.zeros((ROWS, 128))
    weight_rows[:BLOCK, 0] = cell_weight

    def halves(table):
        high = table.astype(ml_dtypes.bfloat16)
        return high, (table - high.astype(np.float64)).astype(ml_dtypes.bfloat16)

    weight_rows[: 2 * FACE, 1] = np.tile(np.concatenate([face_rows, -0.5 * face_rows]), 2)
    fwd_high, fwd_low = halves(forward)
    back_high, back_low = halves(backward)
    again = np.concatenate(halves(forward[: 2 * FACE] @ backward[:, : 2 * FACE]) + (np.zeros((ROWS, ROWS), ml_dtypes.bfloat16),), 1)
    return (
        np.concatenate([np.concatenate([fwd_high, fwd_high, fwd_low], 1), back_high, back_low, again], 0),
        weight_rows.astype(np.float32),
    )


def dot_nn(left, right):
    return jnp.dot(left, right, preferred_element_type=F32)


def dot_nt(left, right):
    return lax.dot_general(left, right, (((1,), (1,)), ((), ())), preferred_element_type=F32)


def split2(value):
    high = value.astype(BF16)
    return high, (value - high.astype(F32)).astype(BF16)


def split3(value):
    high = value.astype(BF16)
    rest = value - high.astype(F32)
    mid = rest.astype(BF16)
    return high, mid, (rest - mid.astype(F32)).astype(BF16)


def far_first(sizes):
    offsets = [tuple(int(i) for i in index) for index in np.ndindex(*sizes) if any(index)]
    offsets.sort(key=lambda index: -sum(min(i, n - i) for i, n in zip(index, sizes)))
    return [index[0] if len(sizes) == 1 else index for index in offsets]


def onehot(index_row, rows, start=0):
    ids = lax.broadcasted_iota(jnp.int32, (rows, index_row.shape[1]), 0) + start
    return jnp.where(ids == index_row, 1.0, 0.0).astype(BF16)


def kernel(
    n_curve, n_group, x_size,
    rs_hbm, cond_hbm, dest_hbm, nb_hbm, ori_hbm, sl_hbm, table_hbm, w_hbm,
    solution_out, residual_out,
    rs_ref, cond_ref, dest_ref, nb_ref, ori_ref, sl_ref, table_ref, w_ref, load_sem,
    b_ref, y_ref, z_ref, fb_ref, tail_ref, x3_ref, q_ref, g_ref, gg_ref, s_ref, sign_ref, f_ref, fs_ref, ch_ref, cl_ref,
    mig_send, mig_recv, far_recv, halo_send, halo_recv, row_send, curve_recv, group_recv,
    mig_ssem, mig_rsem, far_ssem, far_rsem, halo_ssem, halo_rsem, curve_ssem, curve_rsem, group_ssem, group_rsem, one_sem, two_sem, plane_sem,
):
    curve = lax.axis_index("curve")
    group = lax.axis_index("group")
    me = curve * n_group + group
    total = n_curve * n_group
    has_left, has_right = me > 0, me < total - 1
    edge_left, edge_right = (group == 0) & has_left, (group == n_group - 1) & has_right
    plain_left = has_left & jnp.logical_not(edge_left)
    plain_right = has_right & jnp.logical_not(edge_right)
    far_left = (group == 1) & (curve > 0)
    far_right = (group == n_group - 2) & (curve < n_curve - 1)

    def device(rank):
        return (rank // n_group, lax.rem(rank, n_group))

    left, right = device(lax.rem(me + total - 1, total)), device(lax.rem(me + 1, total))
    left_two, right_two = device(lax.rem(me + total - 2, total)), device(lax.rem(me + 2, total))
    z_size = n_group // x_size
    x_pos = lax.rem(group, x_size)
    z_pos = group // x_size
    curve_peers = [(lax.rem(curve + d, n_curve), group) for d in far_first((n_curve,))]
    group_peers = [
        (curve, lax.rem(z_pos + dz, z_size) * x_size + lax.rem(x_pos + dx, x_size))
        for dz, dx in far_first((z_size, x_size))
    ]
    y_size = n_curve // 2
    core = lax.rem(curve, 2)
    core_peer = (curve + 1 - 2 * core, group)

    def along(dim, offset):
        if dim == 0:
            return (curve, z_pos * x_size + lax.rem(x_pos + offset, x_size))
        if dim == 1:
            return (lax.rem(curve + 2 * offset, n_curve), group)
        return (curve, lax.rem(z_pos + offset, z_size) * x_size + x_pos)

    sizes = (x_size, y_size, z_size)
    near_peers = [core_peer] + [
        along(dim, offset) for dim in range(3) for offset in sorted({1, sizes[dim] - 1}) if sizes[dim] > 1
    ]

    def signal(sem, peer):
        pl.semaphore_signal(sem, inc=1, device_id=peer, device_id_type=MESH)

    def spread(reach, ring_sem):
        for dim in range(3):
            if sizes[dim] > 2 * reach + 1:
                signal(ring_sem.at[dim], along(dim, reach))
                signal(ring_sem.at[dim], along(dim, sizes[dim] - reach))

    def gather_known(reach, ring_sem):
        for dim in range(3):
            if sizes[dim] > 2 * reach + 1:
                pl.semaphore_wait(ring_sem.at[dim], 2)

    def two_away():
        gather_known(1, one_sem)
        spread(2, two_sem)

    def whole_plane():
        gather_known(2, two_sem)
        signal(plane_sem.at[0], core_peer)
        for offset in range(1, x_size):
            signal(plane_sem.at[1], along(0, offset))

    def before_sums():
        pl.semaphore_wait(plane_sem.at[0], 1)
        if x_size > 1:
            pl.semaphore_wait(plane_sem.at[1], x_size - 1)

    barrier = pltpu.get_barrier_semaphore()

    @pl.when(has_left)
    def _():
        signal(barrier, left)

    @pl.when(has_right)
    def _():
        signal(barrier, right)

    @pl.when(edge_left)
    def _():
        signal(barrier, left_two)

    @pl.when(edge_right)
    def _():
        signal(barrier, right_two)

    loads = {}
    for i, (name, source, sink) in enumerate(
        (
            ("dest", dest_hbm, dest_ref),
            ("rs", rs_hbm, rs_ref),
            ("cond", cond_hbm, cond_ref),
            ("nb", nb_hbm, nb_ref),
            ("sl", sl_hbm, sl_ref),
            ("ori", ori_hbm, ori_ref),
            ("table", table_hbm, table_ref),
            ("w", w_hbm, w_ref),
        )
    ):
        loads[name] = pltpu.make_async_copy(source, sink, load_sem.at[i])
        loads[name].start()
    for peer in near_peers:
        signal(barrier, peer)

    for start in range(0, CELLS, 64):
        ids = lax.broadcasted_iota(jnp.int32, (64, CELLS), 0) + start
        lanes = lax.broadcasted_iota(jnp.int32, (64, CELLS), 1)
        q_ref[start : start + 64, :] = jnp.where(ids <= lanes, 1.0, 0.0).astype(BF16)

    @pl.when(jnp.logical_not(has_left))
    def _():
        mig_recv[0:MOVE, :] = jnp.zeros((MOVE, ROWS), F32)
        halo_recv[:, 0] = jnp.zeros((2, FACE, GHOST), F32)

    @pl.when(jnp.logical_not(has_right))
    def _():
        mig_recv[MOVE:, :] = jnp.zeros((MOVE, ROWS), F32)
        halo_recv[:, 1] = jnp.zeros((2, FACE, GHOST), F32)

    loads["dest"].wait()

    destination = dest_ref[...]
    target = lax.shift_right_arithmetic(destination, 9) - me
    slot = jnp.bitwise_and(destination, CELLS - 1)
    row8 = lax.broadcasted_iota(jnp.int32, (8, CELLS), 0)
    leaving = jnp.where(((row8 == 0) & (target == -1)) | ((row8 == 1) & (target == 1)), 1.0, 0.0)
    counts = dot_nn(leaving.astype(BF16), q_ref[...]).astype(jnp.int32)
    place = jnp.where(target == -1, counts[0:1] - 1, jnp.where(target == 1, counts[1:2] + (MOVE - 1), -1))
    loads["rs"].wait()
    loads["cond"].wait()
    tail_ref[0:13, :] = rs_ref[112:BLOCK, :]
    tail_ref[13:14, :] = cond_ref[...]
    tail_ref[14:15, :] = (slot + 1).astype(F32)
    tail_ref[15:16, :] = jnp.zeros((1, CELLS), F32)
    for start, stop, value in ((0, 112, rs_ref[0:112, :]), (112, ROWS, tail_ref[...])):
        for i, part in enumerate(split3(value)):
            x3_ref[i * ROWS + start : i * ROWS + stop, :] = part
    packed = dot_nt(onehot(place, 2 * MOVE), x3_ref[...])
    mig_send[...] = packed[:, 0:ROWS] + packed[:, ROWS : 2 * ROWS] + packed[:, 2 * ROWS :]

    greeted = [has_left, has_right, far_left, far_right]
    pl.semaphore_wait(barrier, len(near_peers) + sum(one.astype(jnp.int32) for one in greeted))

    def copy(source, sink, ssem, rsem, peer):
        return pltpu.make_async_remote_copy(
            src_ref=source, dst_ref=sink, send_sem=ssem, recv_sem=rsem, device_id=peer, device_id_type=MESH
        )

    def start_both(to_left, to_right):
        pl.when(has_left)(to_left.start)
        pl.when(has_right)(to_right.start)

    to_left = copy(
        mig_send.at[pl.ds(0, MOVE)], mig_recv.at[pl.ds(MOVE, MOVE)], mig_ssem.at[0], mig_rsem.at[0], left
    )
    to_right = copy(
        mig_send.at[pl.ds(MOVE, MOVE)], mig_recv.at[pl.ds(0, MOVE)], mig_ssem.at[1], mig_rsem.at[1], right
    )
    start_both(to_left, to_right)
    to_far_left = copy(mig_send.at[pl.ds(0, MOVE)], far_recv, far_ssem.at[0], far_rsem, left_two)
    to_far_right = copy(mig_send.at[pl.ds(MOVE, MOVE)], far_recv, far_ssem.at[1], far_rsem, right_two)
    pl.when(far_left)(to_far_left.start)
    pl.when(far_right)(to_far_right.start)
    spread(1, one_sem)
    loads["nb"].wait()
    loads["sl"].wait()
    loads["ori"].wait()

    def project(field, rows=slice(0, 2 * FACE)):
        high, low = field
        return dot_nn(table_ref[rows, 0:256], jnp.concatenate([high, low], 0)) + dot_nn(
            table_ref[rows, 256:384], high
        )

    def stack(face):
        high, low = split2(f_ref[face * FACE : (face + 1) * FACE, :])
        fs_ref[face, 0:FACE, :] = high
        fs_ref[face, FACE : 2 * FACE, :] = low

    def pair(product):
        return product[0:FACE] + product[FACE : 2 * FACE]

    def halo(step):
        return [
            copy(
                halo_send.at[step, side], halo_recv.at[step, 1 - side],
                halo_ssem.at[step, side], halo_rsem.at[step, side], peer,
            )
            for side, peer in ((0, left), (1, right))
        ]

    staying = jnp.where(target == 0, slot, -1)
    for start in range(0, CELLS, 64):
        q_ref[start : start + 64, :] = onehot(staying, 64, start)
    stay = dot_nt(x3_ref[...], q_ref[...])
    y_ref[...] = stay[0:ROWS] + stay[ROWS : 2 * ROWS] + stay[2 * ROWS :]
    for side in range(2):
        for start in range(0, CELLS, 128):
            s_ref[side, start : start + 128, :] = onehot(sl_ref[side : side + 1, :], 128, start)
    loads["table"].wait()
    loads["w"].wait()
    f_ref[0 : 2 * FACE, :] = project(split2(y_ref[...]))
    for side in range(2):
        stack(side)
        halo_send[0, side] = pair(dot_nn(fs_ref[side], s_ref[side]))
        halo_send[0, side, LISTED : LISTED + 1, :] = sl_ref[side : side + 1, :].astype(F32)
    copies_one = halo(0)
    pl.when(edge_left)(copies_one[0].start)
    pl.when(edge_right)(copies_one[1].start)
    mode = lax.broadcasted_iota(jnp.int32, (HALF, CELLS), 0)
    odd_first = jnp.where((mode >= 15) & (mode < 25), 2.0, 0.0)
    second = functools.reduce(jnp.logical_or, [mode == 5 * i + j for i in range(5) for j in (3, 4)])
    odd_second = jnp.where(second, 2.0, 0.0)
    outside = []
    for face in range(6):
        partner = nb_ref[face : face + 1, :]
        outside.append(jnp.where(partner < 0, 2.0, 1.0))
        for start in range(0, CELLS, 64):
            g_ref[face, start : start + 64, :] = onehot(partner, 64, start)
        if face < 2:
            for start in range(0, GHOST, 64):
                gg_ref[face, start : start + 64, :] = onehot(partner, 64, CELLS + face * GHOST + start)
        code = ori_ref[face : face + 1, :]
        first_bit = jnp.bitwise_and(code, 1).astype(F32)
        second_bit = lax.shift_right_arithmetic(code, 1).astype(F32)
        sign_ref[face] = (1.0 - odd_first * first_bit) * (1.0 - odd_second * second_bit)

    two_away()
    pl.when(has_left)(to_right.wait_recv)
    pl.when(has_right)(to_left.wait_recv)

    arrived = mig_recv[...].T
    faces = project(split2(arrived))

    def place_faces(faces, records, listed):
        slots = records[:, BLOCK + 1 : BLOCK + 2].astype(jnp.int32) - 1
        chosen = jnp.where(slots == listed, 1.0, 0.0).astype(BF16)
        return pair(dot_nn(jnp.concatenate(split2(faces), 0), chosen))

    came = mig_recv[...]
    for side, plain in ((0, plain_left), (1, plain_right)):
        more = place_faces(faces[side * FACE : (side + 1) * FACE], came, sl_ref[side : side + 1, :])

        @pl.when(plain)
        def _():
            halo_send[0, side] += more

    pl.when(plain_left)(copies_one[0].start)
    pl.when(plain_right)(copies_one[1].start)

    place_in = arrived[BLOCK + 1 : BLOCK + 2, :].astype(jnp.int32) - 1
    for start in range(0, CELLS, 128):
        q_ref[start : start + 128, 0 : 2 * MOVE] = onehot(place_in, 128, start)
    moved = dot_nt(jnp.concatenate(split3(arrived), 0), q_ref[:, 0 : 2 * MOVE])
    field = y_ref[...] + (moved[0:ROWS] + moved[ROWS : 2 * ROWS] + moved[2 * ROWS :])
    conduct = field[BLOCK : BLOCK + 1, :]
    row_ids = lax.broadcasted_iota(jnp.int32, (ROWS, CELLS), 0)
    b_ref[...] = jnp.where(row_ids < BLOCK, field, 0.0)

    def with_conduct(value):
        return jnp.where(row_ids == BLOCK, conduct, value)

    def coefficients(face, near):
        row = face * FACE
        trace = f_ref[row : row + HALF, :]
        normal = f_ref[row + HALF : row + FACE, :]
        near_conduct = near[25:26, :]
        sign = sign_ref[face]
        near_value = sign * near[0:HALF]
        near_normal = sign * near[HALF:FACE]
        penalty = PENALTY * jnp.maximum(conduct, near_conduct)
        jump = outside[face] * trace - near_value
        first = (
            penalty * jump - (0.5 * outside[face] * conduct) * normal + (0.5 * near_conduct) * near_normal
        )
        parts = (first, conduct * jump)
        for offset, part in zip((0, HALF), parts):
            high, low = split2(part)
            ch_ref[row + offset : row + offset + HALF, :] = high
            cl_ref[row + offset : row + offset + HALF, :] = low
        return parts

    def expand(high, low, columns):
        return (
            dot_nn(high, ch_ref[columns, :])
            + dot_nn(high, cl_ref[columns, :])
            + dot_nn(low, ch_ref[columns, :])
        )

    def backward(start, stop):
        columns = slice(start * FACE, stop * FACE)
        return expand(table_ref[512:640, columns], table_ref[640:768, columns], columns)

    def local_part(value_ref, result_ref):
        for face in range(2, 6):
            stack(face)
        for face in range(2, 6):
            coefficients(face, pair(dot_nn(fs_ref[face ^ 1], g_ref[face])))
        local = [pair(dot_nn(fs_ref[face ^ 1], g_ref[face])) for face in range(2)]
        result_ref[...] = (
            w_ref[:, 0:1] * value_ref[...] + conduct * f_ref[6 * FACE :, :] + backward(2, 6)
        )
        return local

    def complete(face, incoming):
        incoming.wait_recv()
        to_far_left.wait_recv()
        records = jnp.concatenate([mig_send[face * MOVE : (face + 1) * MOVE, :], far_recv[...]], 0)
        other = 1 - face
        faces = project(split2(records.T), slice(other * FACE, (other + 1) * FACE))
        listed = halo_recv[0, face, LISTED : LISTED + 1, :].astype(jnp.int32)
        halo_recv[0, face] += place_faces(faces, records, listed)

    def ghost_part(step, local, copies):
        parts = [(), ()]
        for face in ((0, 1), (1, 0))[step]:
            if step == 0:
                pl.when((plain_left, plain_right)[face])(copies[1 - face].wait_recv)
                pl.when((edge_left, edge_right)[face])(functools.partial(complete, face, copies[1 - face]))
            else:
                pl.when((has_left, has_right)[face])(copies[1 - face].wait_recv)
            high, low = split2(halo_recv[step, face])
            ghost = pair(dot_nn(jnp.concatenate([high, low], 0), gg_ref[face]))
            parts[face] = coefficients(face, local[face] + ghost)
        return parts[0] + parts[1]

    f_ref[...] = project(split2(with_conduct(b_ref[...])), slice(0, 6 * FACE + ROWS))
    fb_ref[...] = f_ref[0 : 2 * FACE, :]
    for side in range(2):
        stack(side)
    local = local_part(b_ref, y_ref)
    faces_ahead = project(split2(with_conduct(y_ref[...])))
    z_ref[...] = faces_ahead
    whole_plane()
    ghost_part(0, local, copies_one)
    f_ref[0 : 2 * FACE, :] = z_ref[...] + expand(
        table_ref[768:896, 0:128], table_ref[768:896, 128:256], slice(0, 2 * FACE)
    )
    copies_two = halo(1)
    for side, there in ((1, has_right), (0, has_left)):
        stack(side)
        halo_send[1, side] = pair(dot_nn(fs_ref[side], s_ref[side]))
        pl.when(there)(copies_two[side].start)

    y_ref[...] += backward(0, 2)
    rest = slice(2 * FACE, 6 * FACE + ROWS)
    f_ref[rest, :] = project(split2(with_conduct(y_ref[...])), rest)
    local = local_part(y_ref, z_ref)

    def summed(terms):
        return jnp.sum(terms, axis=0, keepdims=True)

    source, image, partial = b_ref[...], y_ref[...], z_ref[...]
    early = [summed(source * source), summed(source * image), summed(image * image)]
    late = [summed(source * partial), summed(image * partial)]
    parts = jnp.concatenate(ghost_part(1, local, copies_two), 0) * w_ref[:, 1:2]
    late = [late[0] + summed(fb_ref[...] * parts), late[1] + summed(f_ref[0 : 2 * FACE, :] * parts)]
    lane = lax.broadcasted_iota(jnp.int32, (1, 128), 1)
    row = jnp.zeros((1, 128), F32)
    for index, terms in enumerate(early + late):
        row = row + jnp.where(lane == index, jnp.sum(terms, axis=1, keepdims=True), 0.0)

    before_sums()
    sent = []
    for phase, (peers, landing, ssem, rsem) in enumerate(
        (
            (curve_peers, curve_recv, curve_ssem, curve_rsem),
            (group_peers, group_recv, group_ssem, group_rsem),
        )
    ):
        row_send[phase] = row
        for i, peer in enumerate(peers):
            copy(row_send.at[phase], landing.at[i], ssem, rsem, peer).start()
        if phase == 0:
            z_ref[...] += backward(0, 2)
        every = copy(landing, landing, ssem, rsem, peers[0])
        every.wait_recv()
        terms = [row] + [landing[i] for i in range(len(peers))]
        while len(terms) > 1:
            terms = [sum(terms[i + 1 : i + 2], terms[i]) for i in range(0, len(terms), 2)]
        row = terms[0]
        sent.append(every)

    bb, by, yy, bz, yz = (
        jnp.sum(jnp.where(lane == index, row, 0.0), axis=1, keepdims=True) for index in range(5)
    )
    alpha = bb / by
    norm_next = bb - alpha * (2.0 * by - alpha * yy)
    beta = norm_next / bb
    grow = 1.0 + beta
    curvature = grow * (grow * by - alpha * (bz + yy)) + alpha * (alpha * yz)
    alpha_next = norm_next / curvature
    first = alpha + alpha_next * grow
    second = alpha * alpha_next
    source, image, second_image = b_ref[...], y_ref[...], z_ref[...]
    solution_out[...] = (first * source - second * image)[0:BLOCK]
    residual_out[...] = (source - first * image + second * second_image)[0:BLOCK]
    for one in sent:
        one.wait_send()
    pl.when(far_left)(to_far_left.wait_send)
    pl.when(far_right)(to_far_right.wait_send)
    for one_left, one_right in ((to_left, to_right), copies_one, copies_two):
        pl.when(has_left)(one_left.wait_send)
        pl.when(has_right)(one_right.wait_send)


def write_kernel(solution_ref, residual_ref, solution_out, residual_out, sem):
    copies = [
        pltpu.make_async_copy(solution_ref, solution_out, sem.at[0]),
        pltpu.make_async_copy(residual_ref, residual_out, sem.at[1]),
    ]
    for one in copies:
        one.start()
    for one in copies:
        one.wait()


def solution(mesh):
    n_curve, n_group = mesh.shape["curve"], mesh.shape["group"]
    x_size = min(X_SIZE, n_group)
    constants = tables()
    call = pl.pallas_call(
        functools.partial(kernel, n_curve, n_group, x_size),
        out_shape=(pltpu.VMEM((BLOCK, CELLS), F32), pltpu.VMEM((BLOCK, CELLS), F32)),
        in_specs=[pl.BlockSpec(memory_space=pl.ANY)] * 8,
        out_specs=[pl.BlockSpec(memory_space=pltpu.VMEM)] * 2,
        scratch_shapes=[
            pltpu.VMEM((BLOCK, CELLS), F32),
            pltpu.VMEM((1, CELLS), F32),
            pltpu.VMEM((1, CELLS), jnp.int32),
            pltpu.VMEM((6, CELLS), jnp.int32),
            pltpu.VMEM((6, CELLS), jnp.int32),
            pltpu.VMEM((2, GHOST), jnp.int32),
            *[pltpu.VMEM(table.shape, table.dtype) for table in constants],
            pltpu.SemaphoreType.DMA((8,)),
            pltpu.VMEM((ROWS, CELLS), F32),
            pltpu.VMEM((ROWS, CELLS), F32),
            pltpu.VMEM((ROWS, CELLS), F32),
            pltpu.VMEM((ROWS, CELLS), F32),
            pltpu.VMEM((16, CELLS), F32),
            pltpu.VMEM((3 * ROWS, CELLS), BF16),
            pltpu.VMEM((CELLS, CELLS), BF16),
            pltpu.VMEM((6, CELLS, CELLS), BF16),
            pltpu.VMEM((2, GHOST, CELLS), BF16),
            pltpu.VMEM((2, CELLS, GHOST), BF16),
            pltpu.VMEM((6, HALF, CELLS), F32),
            pltpu.VMEM((6 * FACE + ROWS, CELLS), F32),
            pltpu.VMEM((6, 2 * FACE, CELLS), BF16),
            pltpu.VMEM((6 * FACE, CELLS), BF16),
            pltpu.VMEM((6 * FACE, CELLS), BF16),
            pltpu.VMEM((2 * MOVE, ROWS), F32),
            pltpu.VMEM((2 * MOVE, ROWS), F32),
            pltpu.VMEM((MOVE, ROWS), F32),
            pltpu.VMEM((2, 2, FACE, GHOST), F32),
            pltpu.VMEM((2, 2, FACE, GHOST), F32),
            pltpu.VMEM((2, 1, 128), F32),
            pltpu.VMEM((n_curve - 1, 1, 128), F32),
            pltpu.VMEM((n_group - 1, 1, 128), F32),
            pltpu.SemaphoreType.DMA((2,)),
            pltpu.SemaphoreType.DMA((2,)),
            pltpu.SemaphoreType.DMA((2,)),
            pltpu.SemaphoreType.DMA,
            pltpu.SemaphoreType.DMA((2, 2)),
            pltpu.SemaphoreType.DMA((2, 2)),
            pltpu.SemaphoreType.DMA,
            pltpu.SemaphoreType.DMA,
            pltpu.SemaphoreType.DMA,
            pltpu.SemaphoreType.DMA,
            pltpu.SemaphoreType.REGULAR((3,)),
            pltpu.SemaphoreType.REGULAR((3,)),
            pltpu.SemaphoreType.REGULAR((2,)),
        ],
        compiler_params=pltpu.CompilerParams(collective_id=0, has_side_effects=True),
    )

    field = jax.ShapeDtypeStruct((BLOCK, CELLS), F32)
    write = pl.pallas_call(
        write_kernel,
        out_shape=(field, field),
        in_specs=[pl.BlockSpec(memory_space=pltpu.VMEM)] * 2,
        out_specs=[pl.BlockSpec(memory_space=pl.ANY)] * 2,
        scratch_shapes=[pltpu.SemaphoreType.DMA((2,))],
    )

    def body(right_side, conductivity, destination, neighbour, orientation, send_list):
        fields = call(
            right_side, conductivity[None], destination[None], neighbour, orientation, send_list,
            *[jnp.asarray(table) for table in constants],
        )
        return write(*[pltpu.with_memory_space_constraint(one, pltpu.VMEM) for one in fields])

    in_specs = (
        P(None, CURVE_GROUP),
        P(CURVE_GROUP),
        P(CURVE_GROUP),
        P(None, CURVE_GROUP),
        P(None, CURVE_GROUP),
        P(None, CURVE_GROUP),
    )
    out_specs = (P(None, CURVE_GROUP), P(None, CURVE_GROUP))
    return jax.shard_map(body, mesh=mesh, in_specs=in_specs, out_specs=out_specs, check_vma=False)
```
